512 devices in a mesh: grp: 2 (over y), freq: 32 (over z), beam: 4 (over x), dm: 2 (over core).
Axes of the slice: x: 4, y: 2, z: 32, core: 2. Of those that a mesh axis runs over, the one named last changes fastest.
The devices are a block of a 4x8x32 slice.
Arguments:
- voltages: bfloat16 [32, 256, 16, 2, 1024], P(None, ('freq', 'beam'), ('grp', 'dm')), parts along dimension 2, may hold values from -6 to 6
- grid_feed: int32 [1024], replicated, may hold values from 0 to 1023, each once
- delays: int32 [32, 256, 256], P('freq', None, 'dm'), may hold values from 0 to 4
Outputs:
- dedispersed: float32 [32, 256, 8, 1024], P('freq', 'dm', 'grp', 'beam'), parts along dimension 2
The draws below stay inside these ranges and needn't reach their ends.
There are 2 independent parts, one for each index of `grp`. The reference program is written for one: setup_inputs(seed, part) draws one part's arguments, and reference() takes and returns one part's arrays. A program takes and returns all parts, laid end to end along the dimension named above; an argument that names none is the same for every part. Nothing has to cross between parts.
Inputs may be any that keep to these rules, and one draw needn't show every extreme that they name: `grid_feed`: each feed appears once.
All inputs are finite; a program needn't handle non-finite values.
Results may differ from the reference program's by a relative error of at most 0.0034.
Values may be sent and summed in bfloat16 or wider, within the bound.
No kernel may reach another device: no remote copies, remote signals or barrier semaphores. Data moves between devices by JAX's collectives and lax.ppermute only.
A program may use at most 64 MiB of HBM per device.

```python
import math
import jax
import jax.numpy as jnp
from jax import lax

GX = 4
GY = 256
FEEDS = 1024
FREQS = 8192
DMS = 256
TIME = 8
TOUT = 4
NBAND = 32
SUBS = 256


def draw_delays(key, part):
    deepest = TIME - TOUT
    channels = NBAND * SUBS
    key_value, key_jitter, key_place = jax.random.split(jax.random.fold_in(key, 7), 3)
    position = jnp.arange(channels, dtype=jnp.int32)
    lowered = 2 * channels - position
    quotient = 4 * channels * channels // lowered
    weight = quotient * 1024 // lowered - 1024
    heaviest = jnp.max(weight)
    trial_value = jax.random.randint(key_value, (DMS,), 0, deepest + 1, dtype=jnp.int32)
    forced_dm = jax.random.randint(key_place, (), 0, DMS, dtype=jnp.int32)
    trial_value = jnp.where(jnp.arange(DMS, dtype=jnp.int32) == forced_dm, deepest, trial_value)
    base_delay = trial_value[None, :] * weight[:, None] // heaviest
    jitter = jax.random.randint(key_jitter, (channels, DMS), 0, 2, dtype=jnp.int32)
    return jnp.minimum(base_delay + jitter, deepest).reshape(NBAND, SUBS, DMS).astype(jnp.int32)


def shard_levels(stream_key, shape, cuts, smallest, top_value):
    def one(dim, shards_of):
        heights = jax.random.uniform(jax.random.fold_in(jax.random.fold_in(stream_key, 6), dim), (shards_of,), jnp.float32, smallest / len(cuts), top_value / len(cuts))
        return jnp.repeat(jnp.exp(heights), shape[dim] // shards_of).reshape((-1,) + (1,) * (len(shape) - dim - 1))

    loudness = one(*cuts[0])
    for cut in cuts[1:]:
        loudness = loudness * one(*cut)
    return loudness


def gaussian(rng, shape, spread, bound, cuts=(), kind=jnp.bfloat16):
    loudness = shard_levels(rng, shape, cuts, -0.22, 0.18) if cuts else 1.0
    array = jax.random.normal(rng, shape, jnp.float32) * spread * loudness
    return jnp.minimum(jnp.maximum(array, -bound), bound).astype(kind)


def setup_inputs(seed: int = 0, part: int = 0) -> dict:
    key_list = jax.random.split(jax.random.key(seed), 4)
    part_splits = jax.random.split(jax.random.fold_in(key_list[3], part), 4)
    return {
        "voltages": gaussian(part_splits[0], (NBAND, SUBS, TIME, 2, FEEDS), 1.0, 6.0, ((1, 128), (2, 2))),
        "grid_feed": jax.random.permutation(key_list[1], FEEDS).astype(jnp.int32),
        "delays": draw_delays(jax.random.fold_in(key_list[3], 71), part),
    }


def steering_table(length, factor):
    position = jnp.arange(length, dtype=jnp.int32)
    phase_step = position[:, None] * position[None, :] % length
    phase_angle = phase_step.astype(jnp.float32) * (2.0 * math.pi / length)
    cosine = jnp.cos(phase_angle) * factor
    sine_part = jnp.sin(phase_angle) * factor
    upper_half = jnp.concatenate([cosine, -sine_part], axis=1)
    lower_half = jnp.concatenate([sine_part, cosine], axis=1)
    return jnp.concatenate([upper_half, lower_half], axis=0).astype(jnp.bfloat16)

def quarter_table():
    position = jnp.arange(GX, dtype=jnp.int32)
    phase_step = position[:, None] * position[None, :] % GX
    cosine = jnp.where(phase_step == 0, 1.0, jnp.where(phase_step == 2, -1.0, 0.0)) * 0.5
    sine_part = jnp.where(phase_step == 1, 1.0, jnp.where(phase_step == 3, -1.0, 0.0)) * 0.5
    real_in = jnp.stack([cosine, -sine_part], axis=2)
    imag_in = jnp.stack([sine_part, cosine], axis=2)
    return jnp.stack([real_in, imag_in], axis=1).astype(jnp.float32)

def form_power(voltages, grid_feed):
    row_count = voltages.shape[0] * voltages.shape[1] * voltages.shape[2]
    feed_count = voltages.shape[4]
    gridded = jnp.take(voltages.reshape(row_count, 2, feed_count), grid_feed, axis=2)
    gridded = jnp.transpose(gridded.reshape(row_count, 2, GX, GY), (0, 2, 1, 3)).reshape(row_count * GX, 2 * GY)
    along_y = jnp.dot(gridded, steering_table(GY, 1.0 / math.sqrt(GY)), preferred_element_type=jnp.float32).astype(jnp.bfloat16)
    along_y = along_y.reshape(row_count, GX, 2, GY).astype(jnp.float32)
    formed = jnp.einsum('rgpy,gpbq->rbqy', along_y, quarter_table(), precision=lax.Precision.HIGHEST)
    intensity = 0.5 * (formed[:, :, 0, :] ** 2 + formed[:, :, 1, :] ** 2)
    return intensity.astype(jnp.bfloat16).reshape(row_count, feed_count)

def reference(voltages, grid_feed, delays):
    band_count, sub_count, total_time = (voltages.shape[0], voltages.shape[1], voltages.shape[2])
    feed_count = voltages.shape[4]
    dm_count = delays.shape[2]
    intensity = form_power(voltages, grid_feed).reshape(band_count, sub_count, total_time, feed_count)
    levels = intensity.astype(jnp.float32)
    centered = (levels - lax.optimization_barrier(jnp.mean(levels, axis=2, keepdims=True))).astype(jnp.bfloat16)
    out_time = total_time // 2
    offsets = jnp.arange(out_time, dtype=jnp.int32)
    factor = 1.0 / math.sqrt(FREQS)

    def one_channel(running, entries):
        channel_rows, lag_row = entries
        picked = jnp.take(channel_rows, lag_row[:, None] + offsets[None, :], axis=0)
        return (running + picked.astype(jnp.float32), None)

    def one_band(cumulative, entries):
        band_rows, band_lags = entries
        initial = jnp.zeros((dm_count, out_time, feed_count), jnp.float32)
        band_sum, _ = lax.scan(one_channel, initial, (band_rows, band_lags))
        cumulative = cumulative + band_sum
        return (cumulative, cumulative * factor)
    zeros_start = jnp.zeros((dm_count, out_time, feed_count), jnp.float32)
    _, outputs = lax.scan(one_band, zeros_start, (centered, delays))
    return outputs
```

```python
import math

import jax
import jax.numpy as jnp
from jax import lax
from jax.sharding import PartitionSpec as P

GX = 4
GY = 256
FREQS = 8192


def laid_out(tiles, dim):
    shape = list(tiles.shape[1:])
    shape[dim] *= tiles.shape[0]
    return jnp.moveaxis(tiles, 0, dim).reshape(shape)


def from_everyone(shard, axis):
    copies = jnp.broadcast_to(shard, (lax.axis_size(axis), *shard.shape))
    return lax.all_to_all(copies, axis, split_axis=0, concat_axis=0, tiled=True)


def gathered_copies(shard, axis, dim):
    return laid_out(from_everyone(shard, axis), dim)


def steering_table(length, factor):
    position = jnp.arange(length, dtype=jnp.int32)
    phase_step = position[:, None] * position[None, :] % length
    phase_angle = phase_step.astype(jnp.float32) * (2.0 * math.pi / length)
    cosine = jnp.cos(phase_angle) * factor
    sine_part = jnp.sin(phase_angle) * factor
    upper_half = jnp.concatenate([cosine, -sine_part], axis=1)
    lower_half = jnp.concatenate([sine_part, cosine], axis=1)
    return jnp.concatenate([upper_half, lower_half], axis=0).astype(jnp.bfloat16)


def quarter_table():
    position = jnp.arange(GX, dtype=jnp.int32)
    phase_step = position[:, None] * position[None, :] % GX
    cosine = jnp.where(phase_step == 0, 1.0, jnp.where(phase_step == 2, -1.0, 0.0)) * 0.5
    sine_part = jnp.where(phase_step == 1, 1.0, jnp.where(phase_step == 3, -1.0, 0.0)) * 0.5
    real_in = jnp.stack([cosine, -sine_part], axis=2)
    imag_in = jnp.stack([sine_part, cosine], axis=2)
    return jnp.stack([real_in, imag_in], axis=1).astype(jnp.float32)


def form_power(voltages, grid_feed):
    row_count = voltages.shape[0] * voltages.shape[1] * voltages.shape[2]
    feed_count = voltages.shape[4]
    gridded = jnp.take(voltages.reshape(row_count, 2, feed_count), grid_feed, axis=2)
    gridded = jnp.transpose(gridded.reshape(row_count, 2, GX, GY), (0, 2, 1, 3)).reshape(
        row_count * GX, 2 * GY
    )
    along_y = jnp.dot(
        gridded, steering_table(GY, 1.0 / math.sqrt(GY)), preferred_element_type=jnp.float32
    ).astype(jnp.bfloat16)
    along_y = along_y.reshape(row_count, GX, 2, GY).astype(jnp.float32)
    formed = jnp.einsum("rgpy,gpbq->rbqy", along_y, quarter_table())
    intensity = 0.5 * (formed[:, :, 0, :] ** 2 + formed[:, :, 1, :] ** 2)
    return intensity.astype(jnp.bfloat16).reshape(row_count, feed_count)


def body(voltages, grid_feed, delays):
    band_count, sub_local, time_local = (voltages.shape[0], voltages.shape[1], voltages.shape[2])
    feed_count = voltages.shape[4]
    columns = lax.axis_size("beam")
    col_width = feed_count // columns
    intensity = form_power(voltages, grid_feed).reshape(
        band_count, sub_local, time_local, columns, col_width
    )
    regrouped = jnp.transpose(intensity, (0, 3, 1, 2, 4)).reshape(
        band_count * columns, sub_local, time_local, col_width
    )
    turned = lax.all_to_all(regrouped, ("freq", "beam"), split_axis=0, concat_axis=1, tiled=True)
    turned = turned.reshape(-1, time_local, col_width)
    full_time = gathered_copies(turned, "dm", 1)
    sub_count, total_time = (full_time.shape[0], full_time.shape[1])
    levels = full_time.astype(jnp.float32)
    centered = (levels - jnp.mean(levels, axis=1, keepdims=True)).astype(jnp.bfloat16)
    flattened = centered.reshape(sub_count * total_time, col_width)
    out_time = total_time // 2
    offsets = jnp.arange(out_time, dtype=jnp.int32)
    sample_ids = jnp.arange(total_time, dtype=jnp.int32)
    dm_local = delays.shape[2]
    dm_block = 32
    lag_blocks = jnp.transpose(delays[0]).reshape(dm_local // dm_block, dm_block, sub_count)

    def dedisperse(lag_rows):
        shifted = offsets[None, :, None] + lag_rows[:, None, :]
        selector = (shifted[:, :, :, None] == sample_ids[None, None, None, :]).astype(jnp.bfloat16)
        summed = jnp.dot(
            selector.reshape(dm_block * out_time, sub_count * total_time),
            flattened,
            preferred_element_type=jnp.float32,
        )
        return summed.reshape(dm_block, out_time, col_width)

    partial_sum = lax.map(dedisperse, lag_blocks).reshape(dm_local, out_time, col_width)
    sent = partial_sum.astype(jnp.bfloat16)
    bands = lax.all_to_all(sent[None], "freq", split_axis=1, concat_axis=0, tiled=True)
    sums = jnp.cumsum(bands.astype(jnp.float32), axis=0).astype(jnp.bfloat16)
    cumulative = lax.all_to_all(sums, "freq", split_axis=0, concat_axis=1, tiled=True)
    return cumulative.astype(jnp.float32) * (1.0 / math.sqrt(FREQS))


def solution(mesh):
    in_specs = (P(None, ("freq", "beam"), ("grp", "dm"), None, None), P(), P("freq", None, "dm"))
    out_specs = P("freq", "dm", "grp", "beam")
    return jax.shard_map(body, mesh=mesh, in_specs=in_specs, out_specs=out_specs, check_vma=False)
```

```python
import functools
import math

import jax
import jax.numpy as jnp
import numpy as np
from jax import lax
from jax.experimental import pallas as pl
from jax.experimental.pallas import tpu as pltpu
from jax.sharding import Mesh
from jax.sharding import PartitionSpec as P


GX = 4
GY = 256
FREQS = 8192
LAGS = 5
LANES = 128
BF16 = jnp.bfloat16
F32 = jnp.float32


def steering_table(length):
    position = np.arange(length)
    angle = (position[:, None] * position[None, :] % length) * (2.0 * math.pi / length)
    cosine = np.cos(angle) / math.sqrt(length)
    sine = np.sin(angle) / math.sqrt(length)
    upper = np.concatenate([cosine, -sine], axis=1)
    lower = np.concatenate([sine, cosine], axis=1)
    return np.concatenate([upper, lower], axis=0).astype(BF16)


def iota(shape, dim):
    return lax.broadcasted_iota(jnp.int32, shape, dim)


def lane_blocks(arrays, width, shift):
    count = len(arrays)
    block = iota(arrays[0].shape, 1) // width
    result = None
    for i, array in enumerate(arrays):
        amount = (i - shift) % count * width
        moved = pltpu.roll(array, amount, 1) if amount else array
        result = moved if result is None else jnp.where(block == i, moved, result)
    return result


def front_kernel(times, blocks, near, beams, volt_ref, feed_ref, table_ref, out_ref, along_ref):
    rows, feeds = volt_ref.shape
    half = rows // 2
    chans = half // times
    tall = chans // blocks
    i = iota((rows, rows), 0)
    source = i % chans * (2 * times) + i // chans % times * 2 + i // half
    order = jnp.where(iota((rows, rows), 1) == source, 1.0, 0.0).astype(BF16)
    planes = jnp.dot(order, volt_ref[...], preferred_element_type=F32).astype(BF16)
    pick = jnp.where(iota((feeds, feeds), 0) == feed_ref[...], 1.0, 0.0).astype(BF16)
    grid = jnp.dot(planes, pick, preferred_element_type=F32).astype(BF16)
    for gx in range(GX):
        cells = slice(gx * GY, (gx + 1) * GY)
        paired = jnp.concatenate([grid[:half, cells], grid[half:, cells]], axis=1)
        along = jnp.dot(paired, table_ref[...], preferred_element_type=F32)
        along_ref[gx] = along.astype(BF16)
    per_tile = LANES // beams
    for block in range(blocks):
        for tile in range(GY // LANES):
            power = [[] for _ in range(GX)]
            for t in range(times):
                r = pl.ds(t * chans + block * tall, tall)
                re = [along_ref[gx, r, pl.ds(tile * LANES, LANES)].astype(F32) for gx in range(GX)]
                im = [along_ref[gx, r, pl.ds(GY + tile * LANES, LANES)].astype(F32) for gx in range(GX)]
                er, ei, orr, oi = re[0] + re[2], im[0] + im[2], re[1] + re[3], im[1] + im[3]
                dr, di, ur, ui = re[0] - re[2], im[0] - im[2], re[1] - re[3], im[1] - im[3]
                formed = [(er + orr, ei + oi), (dr + ui, di - ur), (er - orr, ei - oi), (dr - ui, di + ur)]
                for bx, (fr, fi) in enumerate(formed):
                    fr, fi = 0.5 * fr, 0.5 * fi
                    power[bx].append(0.5 * (fr * fr + fi * fi))
            for bx in range(GX):
                for part in range(per_tile):
                    peer = (block * near + tile * per_tile + part) * GX + bx
                    out_ref[peer] = lane_blocks(power[bx], beams, part).astype(BF16)


def dedisperse_kernel(beams, core_ref, own_ref, other_ref, lag_ref, out_ref, level_ref):
    sources, tall, width = own_ref.shape
    bands = out_ref.shape[0]
    subs = tall // bands
    chunk = 8
    low = core_ref[0] == 0

    def center(i, carry):
        mine = own_ref[pl.ds(i * chunk, chunk)].astype(F32).reshape(chunk * tall, width)
        theirs = other_ref[pl.ds(i * chunk, chunk)].astype(F32).reshape(chunk * tall, width)
        early = jnp.where(low, mine, theirs)
        late = jnp.where(low, theirs, mine)
        total = early + late
        amount = width // 2
        while amount >= beams:
            total = total + pltpu.roll(total, amount, 1)
            amount //= 2
        mean = total * (0.5 * beams / width)
        r = pl.ds(pl.multiple_of(i * (chunk * tall), chunk * tall), chunk * tall)
        level_ref[0, r, :] = early - mean
        level_ref[1, r, :] = late - mean
        return carry

    lax.fori_loop(0, sources // chunk, center, 0)
    lane = iota((out_ref.shape[1], width), 1)
    running = None
    for b in range(bands):
        rows = []
        for s in range(subs):
            r = pl.ds(b * subs + s, sources, stride=tall)
            rows.append(jnp.concatenate([level_ref[0, r, :].astype(BF16), level_ref[1, r, :].astype(BF16)], axis=1))
        data = jnp.concatenate(rows, axis=0)
        lags = lag_ref[b].astype(F32)
        chosen = [jnp.where(lags == float(v), 1.0, 0.0).astype(BF16) for v in range(LAGS)]
        for v in range(LAGS):
            picked = jnp.dot(chosen[v], data, preferred_element_type=F32)
            first, second = picked[:, :width], picked[:, width:]
            offset = v * beams
            if offset == 0:
                part = first
            elif offset == width:
                part = second
            else:
                back = width - offset
                part = jnp.where(lane < back, pltpu.roll(first, back, 1), pltpu.roll(second, back, 1))
            running = part if running is None else running + part
        out_ref[b] = running


def spread_kernel(beams, scale, in_ref, out_ref):
    slabs, trials, width = in_ref.shape
    count = width // beams
    for tile in range(slabs // count):
        parts = [in_ref[tile * count + i].astype(F32) * scale for i in range(count)]
        for t in range(count):
            out_ref[pl.ds(tile * count + t, trials, stride=slabs), :] = lane_blocks(parts, beams, t)


def search(voltages, grid_feed, delays):
    bands, sub_local, times = voltages.shape[:3]
    feeds = voltages.shape[4]
    blocks, near, columns = lax.axis_size("far"), lax.axis_size("near"), lax.axis_size("beam")
    peers = blocks * near * columns
    beams = feeds // columns // near
    trials = delays.shape[2]
    subs = delays.shape[1]
    tall = bands // blocks * sub_local
    rows = bands * sub_local * times * 2
    vmem = pl.BlockSpec(memory_space=pltpu.VMEM)

    lag_rows = delays[0].astype(BF16).reshape(peers, sub_local, trials)
    lag_rows = jnp.transpose(lag_rows, (2, 1, 0)).reshape(columns, trials // columns, subs)
    lag_part = lax.dynamic_index_in_dim(lag_rows, lax.axis_index("beam"), 0, keepdims=False)

    sent = pl.pallas_call(
        functools.partial(front_kernel, times, blocks, near, beams),
        out_shape=jax.ShapeDtypeStruct((peers, tall, times * beams), BF16),
        in_specs=[vmem] * 3,
        out_specs=vmem,
        scratch_shapes=[pltpu.VMEM((GX, rows // 2, 2 * GY), BF16)],
        cost_estimate=pl.CostEstimate(flops=2 * 10**9, bytes_accessed=4 * 10**6, transcendentals=0),
        name="front",
    )(voltages.reshape(rows, feeds), grid_feed.reshape(1, feeds), jnp.asarray(steering_table(GY)))
    own = lax.all_to_all(sent, ("far", "near", "beam"), split_axis=0, concat_axis=0, tiled=True)
    lag_near = lax.all_gather(lag_part, "near")
    lags = lax.all_gather(lag_near, "beam")
    lags = jnp.transpose(lags, (1, 0, 2, 3)).reshape(near, trials, subs)
    other = lax.ppermute(own, "dm", [(0, 1), (1, 0)])
    core = lax.axis_index("dm").astype(jnp.int32).reshape(1)
    local = pl.pallas_call(
        functools.partial(dedisperse_kernel, beams),
        out_shape=jax.ShapeDtypeStruct((bands // blocks, trials, times * beams), F32),
        in_specs=[pl.BlockSpec(memory_space=pltpu.SMEM)] + [vmem] * 3,
        out_specs=vmem,
        scratch_shapes=[pltpu.VMEM((2, peers * tall, times * beams), F32)],
        cost_estimate=pl.CostEstimate(flops=2 * 10**9, bytes_accessed=4 * 10**6, transcendentals=0),
        name="dedisperse",
    )(core, own, other, lags)
    total = local[-1]
    base = jnp.zeros_like(total)
    for k in range(blocks - 1):
        message = (base + total).astype(BF16)
        base = base + lax.ppermute(message, "far", [(k, k + 1)]).astype(F32)
    cumulative = (local + base).astype(BF16)
    slabs = lax.all_to_all(cumulative, "near", split_axis=0, concat_axis=0, tiled=True)
    spread = pl.pallas_call(
        functools.partial(spread_kernel, beams, 1.0 / math.sqrt(FREQS)),
        out_shape=jax.ShapeDtypeStruct((trials * near, LANES), F32),
        in_specs=[vmem],
        out_specs=vmem,
        name="spread",
    )(slabs)
    spread = jnp.transpose(spread.reshape(trials, near // times, times, LANES), (0, 2, 1, 3))
    return spread.reshape(1, trials, times, near * beams)


def solution(mesh):
    near = 8
    sizes = mesh.shape
    devices = mesh.devices.reshape(sizes["grp"], sizes["freq"] // near, near, sizes["beam"], sizes["dm"])
    split = Mesh(devices, ("grp", "far", "near", "beam", "dm"))
    freq = ("far", "near")
    in_specs = (P(None, (*freq, "beam"), ("grp", "dm"), None, None), P(), P(freq, None, "dm"))
    out_specs = P(freq, "dm", "grp", "beam")
    return jax.shard_map(search, mesh=split, in_specs=in_specs, out_specs=out_specs, check_vma=False)
```

```python
import functools
import math

import jax
import jax.numpy as jnp
import numpy as np
from jax import lax
from jax.experimental import pallas as pl
from jax.experimental.pallas import tpu as pltpu
from jax.sharding import Mesh
from jax.sharding import PartitionSpec as P


GX = 4
GY = 256
FREQS = 8192
LAGS = 5
LANES = 128
BF16 = jnp.bfloat16
F32 = jnp.float32


def steering_table(length):
    position = np.arange(length)
    angle = (position[:, None] * position[None, :] % length) * (2.0 * math.pi / length)
    cosine = np.cos(angle) / math.sqrt(length)
    sine = np.sin(angle) / math.sqrt(length)
    upper = np.concatenate([cosine, -sine], axis=1)
    lower = np.concatenate([sine, cosine], axis=1)
    return np.concatenate([upper, lower], axis=0).astype(BF16)


def iota(shape, dim):
    return lax.broadcasted_iota(jnp.int32, shape, dim)


def lane_blocks(arrays, width, shift):
    count = len(arrays)
    block = iota(arrays[0].shape, 1) // width
    result = None
    for i, array in enumerate(arrays):
        amount = (i - shift) % count * width
        moved = pltpu.roll(array, amount, 1) if amount else array
        result = moved if result is None else jnp.where(block == i, moved, result)
    return result


def front_kernel(times, blocks, near, beams, volt_ref, feed_ref, table_ref, out_ref, along_ref):
    rows, feeds = 2 * volt_ref.shape[0], volt_ref.shape[2]
    half = rows // 2
    chans = half // times
    tall = chans // blocks
    i = iota((rows, rows), 0)
    source = i % chans * (2 * times) + i // chans % times * 2 + i // half
    order = jnp.where(iota((rows, rows), 1) == source, 1.0, 0.0).astype(BF16)
    planes = jnp.dot(order, volt_ref[...].reshape(rows, feeds), preferred_element_type=F32).astype(BF16)
    pick = jnp.where(iota((feeds, feeds), 0) == feed_ref[...], 1.0, 0.0).astype(BF16)
    grid = jnp.dot(planes, pick, preferred_element_type=F32).astype(BF16)
    for gx in range(GX):
        cells = slice(gx * GY, (gx + 1) * GY)
        paired = jnp.concatenate([grid[:half, cells], grid[half:, cells]], axis=1)
        along = jnp.dot(paired, table_ref[...], preferred_element_type=F32)
        along_ref[gx] = along.astype(BF16)
    per_tile = LANES // beams
    for block in range(blocks):
        for tile in range(GY // LANES):
            power = [[] for _ in range(GX)]
            for t in range(times):
                r = pl.ds(t * chans + block * tall, tall)
                re = [along_ref[gx, r, pl.ds(tile * LANES, LANES)].astype(F32) for gx in range(GX)]
                im = [along_ref[gx, r, pl.ds(GY + tile * LANES, LANES)].astype(F32) for gx in range(GX)]
                er, ei, orr, oi = re[0] + re[2], im[0] + im[2], re[1] + re[3], im[1] + im[3]
                dr, di, ur, ui = re[0] - re[2], im[0] - im[2], re[1] - re[3], im[1] - im[3]
                formed = [(er + orr, ei + oi), (dr + ui, di - ur), (er - orr, ei - oi), (dr - ui, di + ur)]
                for bx, (fr, fi) in enumerate(formed):
                    fr, fi = 0.5 * fr, 0.5 * fi
                    power[bx].append(0.5 * (fr * fr + fi * fi))
            for bx in range(GX):
                for part in range(per_tile):
                    peer = (block * near + tile * per_tile + part) * GX + bx
                    out_ref[peer] = lane_blocks(power[bx], beams, part).astype(BF16)


def dedisperse_kernel(beams, place_ref, own_any, other_any, lag_any, out_ref, total_ref, own_ref, other_ref, lag_ref, level_ref, sems):
    pairs = ((own_any, own_ref), (other_any, other_ref), (lag_any, lag_ref))
    copies = [pltpu.make_async_copy(a, b, sems.at[i]) for i, (a, b) in enumerate(pairs)]
    for copy in copies:
        copy.start()
    for copy in copies:
        copy.wait()
    sources, tall, width = own_ref.shape
    bands = out_ref.shape[0]
    subs = tall // bands
    chunk = 8
    low = place_ref[0] == 0

    def center(i, carry):
        mine = own_ref[pl.ds(i * chunk, chunk)].astype(F32).reshape(chunk * tall, width)
        theirs = other_ref[pl.ds(i * chunk, chunk)].astype(F32).reshape(chunk * tall, width)
        early = jnp.where(low, mine, theirs)
        late = jnp.where(low, theirs, mine)
        total = early + late
        amount = width // 2
        while amount >= beams:
            total = total + pltpu.roll(total, amount, 1)
            amount //= 2
        mean = total * (0.5 * beams / width)
        r = pl.ds(pl.multiple_of(i * (chunk * tall), chunk * tall), chunk * tall)
        level_ref[0, r, :] = early - mean
        level_ref[1, r, :] = late - mean
        return carry

    lax.fori_loop(0, sources // chunk, center, 0)
    lane = iota((out_ref.shape[1], width), 1)
    running = None
    for b in range(bands):
        rows = []
        for s in range(subs):
            r = pl.ds(b * subs + s, sources, stride=tall)
            rows.append(jnp.concatenate([level_ref[0, r, :].astype(BF16), level_ref[1, r, :].astype(BF16)], axis=1))
        data = jnp.concatenate(rows, axis=0)
        lags = lag_ref[lax.rem(b + bands - place_ref[1], bands)].astype(F32)
        chosen = [jnp.where(lags == float(v), 1.0, 0.0).astype(BF16) for v in range(LAGS)]
        for v in range(LAGS):
            picked = jnp.dot(chosen[v], data, preferred_element_type=F32)
            first, second = picked[:, :width], picked[:, width:]
            offset = v * beams
            if offset == 0:
                part = first
            elif offset == width:
                part = second
            else:
                back = width - offset
                part = jnp.where(lane < back, pltpu.roll(first, back, 1), pltpu.roll(second, back, 1))
            running = part if running is None else running + part
        out_ref[b] = running
    total_ref[...] = running


def spread_kernel(beams, scale, in_ref, out_ref):
    slabs, trials, width = in_ref.shape
    count = width // beams
    for tile in range(slabs // count):
        parts = [in_ref[tile * count + i].astype(F32) * scale for i in range(count)]
        for t in range(count):
            out_ref[pl.ds(tile * count + t, trials, stride=slabs), :] = lane_blocks(parts, beams, t)


def search(voltages, grid_feed, delays):
    bands, sub_local, times = voltages.shape[:3]
    feeds = voltages.shape[4]
    blocks, near, columns = lax.axis_size("far"), lax.axis_size("near"), lax.axis_size("beam")
    peers = blocks * near * columns
    beams = feeds // columns // near
    trials = delays.shape[2]
    subs = delays.shape[1]
    tall = bands // blocks * sub_local
    rows = bands * sub_local * times * 2
    vmem = pl.BlockSpec(memory_space=pltpu.VMEM)

    lag_rows = delays[0].astype(BF16).reshape(peers, sub_local, trials)
    lag_rows = jnp.transpose(lag_rows, (2, 1, 0)).reshape(trials, subs)

    sent = pl.pallas_call(
        functools.partial(front_kernel, times, blocks, near, beams),
        out_shape=jax.ShapeDtypeStruct((peers, tall, times * beams), BF16),
        in_specs=[vmem] * 3,
        out_specs=vmem,
        scratch_shapes=[pltpu.VMEM((GX, rows // 2, 2 * GY), BF16)],
        cost_estimate=pl.CostEstimate(flops=2 * 10**9, bytes_accessed=4 * 10**6, transcendentals=0),
        name="front",
    )(voltages.reshape(rows // 2, 2, feeds), grid_feed.reshape(1, feeds), jnp.asarray(steering_table(GY)))
    own = lax.all_to_all(sent, ("far", "near", "beam"), split_axis=0, concat_axis=0, tiled=True)
    share = near // columns
    fetched = []
    for j in range(share):
        steps = [(n, x, (n + x * share + j) % near) for n in range(near) for x in range(columns)]
        pairs = [(source * columns + x, n * columns + x) for n, x, source in steps]
        fetched.append(lax.ppermute(lag_rows, ("near", "beam"), pairs))
    lags = lax.all_gather(jnp.stack(fetched), "beam").reshape(near, trials, subs)
    other = lax.ppermute(own, "dm", [(0, 1), (1, 0)])
    place = jnp.stack([lax.axis_index("dm"), lax.axis_index("near")]).astype(jnp.int32)
    anywhere = pl.BlockSpec(memory_space=pl.ANY)
    local, total = pl.pallas_call(
        functools.partial(dedisperse_kernel, beams),
        out_shape=(
            jax.ShapeDtypeStruct((bands // blocks, trials, times * beams), F32),
            jax.ShapeDtypeStruct((trials, times * beams), F32),
        ),
        in_specs=[pl.BlockSpec(memory_space=pltpu.SMEM)] + [anywhere] * 3,
        out_specs=(vmem, vmem),
        scratch_shapes=[
            pltpu.VMEM(own.shape, BF16),
            pltpu.VMEM(own.shape, BF16),
            pltpu.VMEM(lags.shape, BF16),
            pltpu.VMEM((2, peers * tall, times * beams), F32),
            pltpu.SemaphoreType.DMA((3,)),
        ],
        compiler_params=pltpu.CompilerParams(vmem_limit_bytes=24 * 2**20),
        cost_estimate=pl.CostEstimate(flops=2 * 10**9, bytes_accessed=4 * 10**6, transcendentals=0),
        name="dedisperse",
    )(place, own, other, lags)
    base = jnp.zeros_like(total)
    for k in range(blocks - 1):
        message = (base + total).astype(BF16)
        base = base + lax.ppermute(message, "far", [(k, k + 1)]).astype(F32)
    cumulative = (local + base).astype(BF16)
    slabs = lax.all_to_all(cumulative, "near", split_axis=0, concat_axis=0, tiled=True)
    spread = pl.pallas_call(
        functools.partial(spread_kernel, beams, 1.0 / math.sqrt(FREQS)),
        out_shape=jax.ShapeDtypeStruct((trials * near, LANES), F32),
        in_specs=[vmem],
        out_specs=vmem,
        name="spread",
    )(slabs)
    spread = jnp.transpose(spread.reshape(trials, near // times, times, LANES), (0, 2, 1, 3))
    return spread.reshape(1, trials, times, near * beams)


def solution(mesh):
    near = 8
    sizes = mesh.shape
    devices = mesh.devices.reshape(sizes["grp"], sizes["freq"] // near, near, sizes["beam"], sizes["dm"])
    split = Mesh(devices, ("grp", "far", "near", "beam", "dm"))
    freq = ("far", "near")
    in_specs = (P(None, (*freq, "beam"), ("grp", "dm"), None, None), P(), P(freq, None, "dm"))
    out_specs = P(freq, "dm", "grp", "beam")
    return jax.shard_map(search, mesh=split, in_specs=in_specs, out_specs=out_specs, check_vma=False)
```

```python
import functools
import math

import jax
import jax.numpy as jnp
import numpy as np
from jax import lax
from jax.experimental import pallas as pl
from jax.experimental.pallas import tpu as pltpu
from jax.sharding import Mesh
from jax.sharding import PartitionSpec as P


GX = 4
GY = 256
FREQS = 8192
LAGS = 5
LANES = 128
BF16 = jnp.bfloat16
F32 = jnp.float32


def steering_table(length):
    position = np.arange(length)
    angle = (position[:, None] * position[None, :] % length) * (2.0 * math.pi / length)
    cosine = np.cos(angle) / math.sqrt(length)
    sine = np.sin(angle) / math.sqrt(length)
    upper = np.concatenate([cosine, -sine], axis=1)
    lower = np.concatenate([sine, cosine], axis=1)
    return np.concatenate([upper, lower], axis=0).astype(BF16)


def iota(shape, dim):
    return lax.broadcasted_iota(jnp.int32, shape, dim)


def lane_blocks(arrays, width, shift):
    count = len(arrays)
    block = iota(arrays[0].shape, 1) // width
    result = None
    for i, array in enumerate(arrays):
        amount = (i - shift) % count * width
        moved = pltpu.roll(array, amount, 1) if amount else array
        result = moved if result is None else jnp.where(block == i, moved, result)
    return result


def front_kernel(times, blocks, near, beams, volt_any, feed_ref, table_any, out_ref, volt_ref, table_ref, along_ref, sems):
    load = pltpu.make_async_copy(volt_any, volt_ref, sems.at[0])
    load_table = pltpu.make_async_copy(table_any, table_ref, sems.at[1])
    load.start()
    load_table.start()
    rows, feeds = 2 * volt_ref.shape[0], volt_ref.shape[2]
    half = rows // 2
    chans = half // times
    tall = chans // blocks
    i = iota((rows, rows), 0)
    source = i % chans * (2 * times) + i // chans % times * 2 + i // half
    order = jnp.where(iota((rows, rows), 1) == source, 1.0, 0.0).astype(BF16)
    pick = jnp.where(iota((feeds, feeds), 0) == feed_ref[...], 1.0, 0.0).astype(BF16)
    load.wait()
    load_table.wait()
    planes = jnp.dot(order, volt_ref[...].reshape(rows, feeds), preferred_element_type=F32).astype(BF16)
    grid = jnp.dot(planes, pick, preferred_element_type=F32).astype(BF16)
    for gx in range(GX):
        cells = slice(gx * GY, (gx + 1) * GY)
        paired = jnp.concatenate([grid[:half, cells], grid[half:, cells]], axis=1)
        along = jnp.dot(paired, table_ref[...], preferred_element_type=F32)
        along_ref[gx] = along.astype(BF16)
    per_tile = LANES // beams
    for block in range(blocks):
        for tile in range(GY // LANES):
            power = [[] for _ in range(GX)]
            for t in range(times):
                r = pl.ds(t * chans + block * tall, tall)
                re = [along_ref[gx, r, pl.ds(tile * LANES, LANES)].astype(F32) for gx in range(GX)]
                im = [along_ref[gx, r, pl.ds(GY + tile * LANES, LANES)].astype(F32) for gx in range(GX)]
                er, ei, orr, oi = re[0] + re[2], im[0] + im[2], re[1] + re[3], im[1] + im[3]
                dr, di, ur, ui = re[0] - re[2], im[0] - im[2], re[1] - re[3], im[1] - im[3]
                formed = [(er + orr, ei + oi), (dr + ui, di - ur), (er - orr, ei - oi), (dr - ui, di + ur)]
                for bx, (fr, fi) in enumerate(formed):
                    fr, fi = 0.5 * fr, 0.5 * fi
                    power[bx].append(0.5 * (fr * fr + fi * fi))
            for bx in range(GX):
                for part in range(per_tile):
                    peer = (block * near + tile * per_tile + part) * GX + bx
                    out_ref[peer] = lane_blocks(power[bx], beams, part).astype(BF16)


def dedisperse_kernel(beams, place_ref, own_any, other_any, lag_any, out_ref, total_ref, own_ref, other_ref, lag_ref, level_ref, sems):
    pairs = ((own_any, own_ref), (other_any, other_ref), (lag_any, lag_ref))
    copies = [pltpu.make_async_copy(a, b, sems.at[i]) for i, (a, b) in enumerate(pairs)]
    for copy in copies:
        copy.start()
    for copy in copies:
        copy.wait()
    sources, tall, width = own_ref.shape
    bands = out_ref.shape[0]
    subs = tall // bands
    chunk = 8
    low = place_ref[0] == 0

    def center(i, carry):
        mine = own_ref[pl.ds(i * chunk, chunk)].astype(F32).reshape(chunk * tall, width)
        theirs = other_ref[pl.ds(i * chunk, chunk)].astype(F32).reshape(chunk * tall, width)
        early = jnp.where(low, mine, theirs)
        late = jnp.where(low, theirs, mine)
        total = early + late
        amount = width // 2
        while amount >= beams:
            total = total + pltpu.roll(total, amount, 1)
            amount //= 2
        mean = total * (0.5 * beams / width)
        r = pl.ds(pl.multiple_of(i * (chunk * tall), chunk * tall), chunk * tall)
        level_ref[0, r, :] = early - mean
        level_ref[1, r, :] = late - mean
        return carry

    lax.fori_loop(0, sources // chunk, center, 0)
    lane = iota((out_ref.shape[1], width), 1)
    running = None
    for b in range(bands):
        rows = []
        for s in range(subs):
            r = pl.ds(b * subs + s, sources, stride=tall)
            rows.append(jnp.concatenate([level_ref[0, r, :].astype(BF16), level_ref[1, r, :].astype(BF16)], axis=1))
        data = jnp.concatenate(rows, axis=0)
        lags = lag_ref[lax.rem(b + bands - place_ref[1], bands)].astype(F32)
        chosen = [jnp.where(lags == float(v), 1.0, 0.0).astype(BF16) for v in range(LAGS)]
        for v in range(LAGS):
            picked = jnp.dot(chosen[v], data, preferred_element_type=F32)
            first, second = picked[:, :width], picked[:, width:]
            offset = v * beams
            if offset == 0:
                part = first
            elif offset == width:
                part = second
            else:
                back = width - offset
                part = jnp.where(lane < back, pltpu.roll(first, back, 1), pltpu.roll(second, back, 1))
            running = part if running is None else running + part
        out_ref[b] = running
    total_ref[...] = running


def spread_kernel(beams, scale, in_any, out_ref, in_ref, sem):
    copy = pltpu.make_async_copy(in_any, in_ref, sem)
    copy.start()
    copy.wait()
    slabs, trials, width = in_ref.shape
    count = width // beams
    for tile in range(slabs // count):
        parts = [in_ref[tile * count + i].astype(F32) * scale for i in range(count)]
        for t in range(count):
            out_ref[pl.ds(tile * count + t, trials, stride=slabs), :] = lane_blocks(parts, beams, t)


def search(voltages, grid_feed, delays):
    bands, sub_local, times = voltages.shape[:3]
    feeds = voltages.shape[4]
    blocks, near, columns = lax.axis_size("far"), lax.axis_size("near"), lax.axis_size("beam")
    peers = blocks * near * columns
    beams = feeds // columns // near
    trials = delays.shape[2]
    subs = delays.shape[1]
    tall = bands // blocks * sub_local
    rows = bands * sub_local * times * 2
    vmem = pl.BlockSpec(memory_space=pltpu.VMEM)
    anywhere = pl.BlockSpec(memory_space=pl.ANY)

    lag_rows = delays[0].astype(BF16).reshape(peers, sub_local, trials)
    lag_rows = jnp.transpose(lag_rows, (2, 1, 0)).reshape(trials, subs)

    sent = pl.pallas_call(
        functools.partial(front_kernel, times, blocks, near, beams),
        out_shape=jax.ShapeDtypeStruct((peers, tall, times * beams), BF16),
        in_specs=[anywhere, vmem, anywhere],
        out_specs=vmem,
        scratch_shapes=[
            pltpu.VMEM((rows // 2, 2, feeds), BF16),
            pltpu.VMEM((2 * GY, 2 * GY), BF16),
            pltpu.VMEM((GX, rows // 2, 2 * GY), BF16),
            pltpu.SemaphoreType.DMA((2,)),
        ],
        cost_estimate=pl.CostEstimate(flops=2 * 10**9, bytes_accessed=4 * 10**6, transcendentals=0),
        name="front",
    )(voltages.reshape(rows // 2, 2, feeds), grid_feed.reshape(1, feeds), jnp.asarray(steering_table(GY)))
    own = lax.all_to_all(sent, ("far", "near", "beam"), split_axis=0, concat_axis=0, tiled=True)
    share = near // columns
    fetched = []
    for j in range(share):
        steps = [(n, x, (n + x * share + j) % near) for n in range(near) for x in range(columns)]
        pairs = [(source * columns + x, n * columns + x) for n, x, source in steps]
        fetched.append(lax.ppermute(lag_rows, ("near", "beam"), pairs))
    lags = lax.all_gather(jnp.stack(fetched), "beam").reshape(near, trials, subs)
    other = lax.ppermute(own, "dm", [(0, 1), (1, 0)])
    place = jnp.stack([lax.axis_index("dm"), lax.axis_index("near")]).astype(jnp.int32)
    local, total = pl.pallas_call(
        functools.partial(dedisperse_kernel, beams),
        out_shape=(
            jax.ShapeDtypeStruct((bands // blocks, trials, times * beams), F32),
            jax.ShapeDtypeStruct((trials, times * beams), F32),
        ),
        in_specs=[pl.BlockSpec(memory_space=pltpu.SMEM)] + [anywhere] * 3,
        out_specs=(vmem, vmem),
        scratch_shapes=[
            pltpu.VMEM(own.shape, BF16),
            pltpu.VMEM(own.shape, BF16),
            pltpu.VMEM(lags.shape, BF16),
            pltpu.VMEM((2, peers * tall, times * beams), F32),
            pltpu.SemaphoreType.DMA((3,)),
        ],
        compiler_params=pltpu.CompilerParams(vmem_limit_bytes=24 * 2**20),
        cost_estimate=pl.CostEstimate(flops=2 * 10**9, bytes_accessed=4 * 10**6, transcendentals=0),
        name="dedisperse",
    )(place, own, other, lags)
    base = jnp.zeros_like(total)
    for k in range(blocks - 1):
        message = (base + total).astype(BF16)
        base = base + lax.ppermute(message, "far", [(k, k + 1)]).astype(F32)
    cumulative = (local + base).astype(BF16)
    slabs = lax.all_to_all(cumulative, "near", split_axis=0, concat_axis=0, tiled=True)
    spread = pl.pallas_call(
        functools.partial(spread_kernel, beams, 1.0 / math.sqrt(FREQS)),
        out_shape=jax.ShapeDtypeStruct((trials * near, LANES), F32),
        in_specs=[anywhere],
        out_specs=vmem,
        scratch_shapes=[pltpu.VMEM(slabs.shape, BF16), pltpu.SemaphoreType.DMA],
        compiler_params=pltpu.CompilerParams(vmem_limit_bytes=24 * 2**20),
        name="spread",
    )(slabs)
    spread = jnp.transpose(spread.reshape(trials, near // times, times, LANES), (0, 2, 1, 3))
    return spread.reshape(1, trials, times, near * beams)


def solution(mesh):
    near = 8
    sizes = mesh.shape
    devices = mesh.devices.reshape(sizes["grp"], sizes["freq"] // near, near, sizes["beam"], sizes["dm"])
    split = Mesh(devices, ("grp", "far", "near", "beam", "dm"))
    freq = ("far", "near")
    in_specs = (P(None, (*freq, "beam"), ("grp", "dm"), None, None), P(), P(freq, None, "dm"))
    out_specs = P(freq, "dm", "grp", "beam")
    return jax.shard_map(search, mesh=split, in_specs=in_specs, out_specs=out_specs, check_vma=False)
```

```python
import functools
import math

import jax
import jax.numpy as jnp
import numpy as np
from jax import lax
from jax.experimental import pallas as pl
from jax.experimental.pallas import tpu as pltpu
from jax.sharding import Mesh
from jax.sharding import PartitionSpec as P


GX = 4
GY = 256
FREQS = 8192
LAGS = 5
LANES = 128
BF16 = jnp.bfloat16
F32 = jnp.float32


def steering_table(length):
    position = np.arange(length)
    angle = (position[:, None] * position[None, :] % length) * (2.0 * math.pi / length)
    cosine = np.cos(angle) / math.sqrt(length)
    sine = np.sin(angle) / math.sqrt(length)
    upper = np.concatenate([cosine, -sine], axis=1)
    lower = np.concatenate([sine, cosine], axis=1)
    return np.concatenate([upper, lower], axis=0).astype(BF16)


def iota(shape, dim):
    return lax.broadcasted_iota(jnp.int32, shape, dim)


def lane_blocks(arrays, width, shift):
    count = len(arrays)
    block = iota(arrays[0].shape, 1) // width
    result = None
    for i, array in enumerate(arrays):
        amount = (i - shift) % count * width
        moved = pltpu.roll(array, amount, 1) if amount else array
        result = moved if result is None else jnp.where(block == i, moved, result)
    return result


def front_kernel(times, blocks, near, beams, volt_any, feed_ref, table_any, out_ref, volt_ref, table_ref, along_ref, sems):
    load = pltpu.make_async_copy(volt_any, volt_ref, sems.at[0])
    load_table = pltpu.make_async_copy(table_any, table_ref, sems.at[1])
    load.start()
    load_table.start()
    rows, feeds = 2 * volt_ref.shape[0], volt_ref.shape[2]
    half = rows // 2
    chans = half // times
    tall = chans // blocks
    i = iota((rows, rows), 0)
    source = i % chans * (2 * times) + i // chans % times * 2 + i // half
    order = jnp.where(iota((rows, rows), 1) == source, 1.0, 0.0).astype(BF16)
    pick = jnp.where(iota((feeds, feeds), 0) == feed_ref[...], 1.0, 0.0).astype(BF16)
    load.wait()
    load_table.wait()
    planes = jnp.dot(order, volt_ref[...].reshape(rows, feeds), preferred_element_type=F32).astype(BF16)
    grid = jnp.dot(planes, pick, preferred_element_type=F32).astype(BF16)
    for gx in range(GX):
        cells = slice(gx * GY, (gx + 1) * GY)
        paired = jnp.concatenate([grid[:half, cells], grid[half:, cells]], axis=1)
        along = jnp.dot(paired, table_ref[...], preferred_element_type=F32)
        along_ref[gx] = along.astype(BF16)
    per_tile = LANES // beams
    for block in range(blocks):
        for tile in range(GY // LANES):
            power = [[] for _ in range(GX)]
            for t in range(times):
                r = pl.ds(t * chans + block * tall, tall)
                re = [along_ref[gx, r, pl.ds(tile * LANES, LANES)].astype(F32) for gx in range(GX)]
                im = [along_ref[gx, r, pl.ds(GY + tile * LANES, LANES)].astype(F32) for gx in range(GX)]
                er, ei, orr, oi = re[0] + re[2], im[0] + im[2], re[1] + re[3], im[1] + im[3]
                dr, di, ur, ui = re[0] - re[2], im[0] - im[2], re[1] - re[3], im[1] - im[3]
                formed = [(er + orr, ei + oi), (dr + ui, di - ur), (er - orr, ei - oi), (dr - ui, di + ur)]
                for bx, (fr, fi) in enumerate(formed):
                    fr, fi = 0.5 * fr, 0.5 * fi
                    power[bx].append(0.5 * (fr * fr + fi * fi))
            for bx in range(GX):
                for part in range(per_tile):
                    peer = (block * near + tile * per_tile + part) * GX + bx
                    out_ref[peer] = lane_blocks(power[bx], beams, part).astype(BF16)


def dedisperse_kernel(beams, place_ref, own_any, other_any, lag_any, out_ref, total_ref, own_ref, other_ref, lag_ref, level_ref, sems):
    columns, share = lag_ref.shape[:2]
    pairs = ((own_any, own_ref), (other_any, other_ref), (lag_any, lag_ref))
    copies = [pltpu.make_async_copy(a, b, sems.at[i]) for i, (a, b) in enumerate(pairs)]
    for copy in copies:
        copy.start()
    for copy in copies:
        copy.wait()
    sources, tall, width = own_ref.shape
    bands = out_ref.shape[0]
    subs = tall // bands
    chunk = 8
    low = place_ref[0] == 0

    def center(i, carry):
        mine = own_ref[pl.ds(i * chunk, chunk)].astype(F32).reshape(chunk * tall, width)
        theirs = other_ref[pl.ds(i * chunk, chunk)].astype(F32).reshape(chunk * tall, width)
        early = jnp.where(low, mine, theirs)
        late = jnp.where(low, theirs, mine)
        total = early + late
        amount = width // 2
        while amount >= beams:
            total = total + pltpu.roll(total, amount, 1)
            amount //= 2
        mean = total * (0.5 * beams / width)
        r = pl.ds(pl.multiple_of(i * (chunk * tall), chunk * tall), chunk * tall)
        level_ref[0, r, :] = early - mean
        level_ref[1, r, :] = late - mean
        return carry

    lax.fori_loop(0, sources // chunk, center, 0)
    lane = iota((out_ref.shape[1], width), 1)
    running = None
    for b in range(bands):
        rows = []
        for s in range(subs):
            r = pl.ds(b * subs + s, sources, stride=tall)
            rows.append(jnp.concatenate([level_ref[0, r, :].astype(BF16), level_ref[1, r, :].astype(BF16)], axis=1))
        data = jnp.concatenate(rows, axis=0)
        turn = lax.rem(b + bands - place_ref[1], bands)
        column = lax.rem(lax.div(turn, share) + columns - place_ref[2], columns)
        lags = lag_ref[column, lax.rem(turn, share)].astype(F32)
        chosen = [jnp.where(lags == float(v), 1.0, 0.0).astype(BF16) for v in range(LAGS)]
        for v in range(LAGS):
            picked = jnp.dot(chosen[v], data, preferred_element_type=F32)
            first, second = picked[:, :width], picked[:, width:]
            offset = v * beams
            if offset == 0:
                part = first
            elif offset == width:
                part = second
            else:
                back = width - offset
                part = jnp.where(lane < back, pltpu.roll(first, back, 1), pltpu.roll(second, back, 1))
            running = part if running is None else running + part
        out_ref[b] = running
    total_ref[...] = running


def spread_kernel(beams, scale, in_any, out_ref, in_ref, sem):
    copy = pltpu.make_async_copy(in_any, in_ref, sem)
    copy.start()
    copy.wait()
    slabs, trials, width = in_ref.shape
    count = width // beams
    for tile in range(slabs // count):
        parts = [in_ref[tile * count + i].astype(F32) * scale for i in range(count)]
        for t in range(count):
            out_ref[pl.ds(tile * count + t, trials, stride=slabs), :] = lane_blocks(parts, beams, t)


def search(voltages, grid_feed, delays):
    bands, sub_local, times = voltages.shape[:3]
    feeds = voltages.shape[4]
    blocks, near, columns = lax.axis_size("far"), lax.axis_size("near"), lax.axis_size("beam")
    peers = blocks * near * columns
    beams = feeds // columns // near
    trials = delays.shape[2]
    subs = delays.shape[1]
    tall = bands // blocks * sub_local
    rows = bands * sub_local * times * 2
    vmem = pl.BlockSpec(memory_space=pltpu.VMEM)
    anywhere = pl.BlockSpec(memory_space=pl.ANY)

    lag_rows = delays[0].astype(BF16).reshape(peers, sub_local, trials)
    lag_rows = jnp.transpose(lag_rows, (2, 1, 0)).reshape(trials, subs)

    sent = pl.pallas_call(
        functools.partial(front_kernel, times, blocks, near, beams),
        out_shape=jax.ShapeDtypeStruct((peers, tall, times * beams), BF16),
        in_specs=[anywhere, vmem, anywhere],
        out_specs=vmem,
        scratch_shapes=[
            pltpu.VMEM((rows // 2, 2, feeds), BF16),
            pltpu.VMEM((2 * GY, 2 * GY), BF16),
            pltpu.VMEM((GX, rows // 2, 2 * GY), BF16),
            pltpu.SemaphoreType.DMA((2,)),
        ],
        cost_estimate=pl.CostEstimate(flops=2 * 10**9, bytes_accessed=4 * 10**6, transcendentals=0),
        name="front",
    )(voltages.reshape(rows // 2, 2, feeds), grid_feed.reshape(1, feeds), jnp.asarray(steering_table(GY)))
    own = lax.all_to_all(sent, ("far", "near", "beam"), split_axis=0, concat_axis=0, tiled=True)
    share = near // columns
    fetched = []
    for j in range(share):
        steps = [(n, x, (n + x * share + j) % near) for n in range(near) for x in range(columns)]
        pairs = [(source * columns + x, n * columns + x) for n, x, source in steps]
        fetched.append(lax.ppermute(lag_rows, ("near", "beam"), pairs))
    lags = [jnp.stack(fetched)]
    for step in range(1, columns):
        pairs = [((x + step) % columns, x) for x in range(columns)]
        lags.append(lax.ppermute(lags[0], "beam", pairs))
    lags = jnp.stack(lags)
    other = lax.ppermute(own, "dm", [(0, 1), (1, 0)])
    place = jnp.stack([lax.axis_index(name) for name in ("dm", "near", "beam")]).astype(jnp.int32)
    local, total = pl.pallas_call(
        functools.partial(dedisperse_kernel, beams),
        out_shape=(
            jax.ShapeDtypeStruct((bands // blocks, trials, times * beams), F32),
            jax.ShapeDtypeStruct((trials, times * beams), F32),
        ),
        in_specs=[pl.BlockSpec(memory_space=pltpu.SMEM)] + [anywhere] * 3,
        out_specs=(vmem, vmem),
        scratch_shapes=[
            pltpu.VMEM(own.shape, BF16),
            pltpu.VMEM(own.shape, BF16),
            pltpu.VMEM(lags.shape, BF16),
            pltpu.VMEM((2, peers * tall, times * beams), F32),
            pltpu.SemaphoreType.DMA((3,)),
        ],
        compiler_params=pltpu.CompilerParams(vmem_limit_bytes=24 * 2**20),
        cost_estimate=pl.CostEstimate(flops=2 * 10**9, bytes_accessed=4 * 10**6, transcendentals=0),
        name="dedisperse",
    )(place, own, other, lags)
    base = jnp.zeros_like(total)
    for k in range(blocks - 1):
        message = (base + total).astype(BF16)
        base = base + lax.ppermute(message, "far", [(k, k + 1)]).astype(F32)
    cumulative = (local + base).astype(BF16)
    slabs = lax.all_to_all(cumulative, "near", split_axis=0, concat_axis=0, tiled=True)
    spread = pl.pallas_call(
        functools.partial(spread_kernel, beams, 1.0 / math.sqrt(FREQS)),
        out_shape=jax.ShapeDtypeStruct((trials * near, LANES), F32),
        in_specs=[anywhere],
        out_specs=vmem,
        scratch_shapes=[pltpu.VMEM(slabs.shape, BF16), pltpu.SemaphoreType.DMA],
        compiler_params=pltpu.CompilerParams(vmem_limit_bytes=24 * 2**20),
        name="spread",
    )(slabs)
    spread = jnp.transpose(spread.reshape(trials, near // times, times, LANES), (0, 2, 1, 3))
    return spread.reshape(1, trials, times, near * beams)


def solution(mesh):
    near = 8
    sizes = mesh.shape
    devices = mesh.devices.reshape(sizes["grp"], sizes["freq"] // near, near, sizes["beam"], sizes["dm"])
    split = Mesh(devices, ("grp", "far", "near", "beam", "dm"))
    freq = ("far", "near")
    in_specs = (P(None, (*freq, "beam"), ("grp", "dm"), None, None), P(), P(freq, None, "dm"))
    out_specs = P(freq, "dm", "grp", "beam")
    return jax.shard_map(search, mesh=split, in_specs=in_specs, out_specs=out_specs, check_vma=False)
```

```python
import functools
import math

import jax
import jax.numpy as jnp
import numpy as np
from jax import lax
from jax.experimental import pallas as pl
from jax.experimental.pallas import tpu as pltpu
from jax.sharding import Mesh
from jax.sharding import PartitionSpec as P


GX = 4
GY = 256
FREQS = 8192
LAGS = 5
LANES = 128
BF16 = jnp.bfloat16
F32 = jnp.float32


def steering_table(length):
    position = np.arange(length)
    angle = (position[:, None] * position[None, :] % length) * (2.0 * math.pi / length)
    cosine = np.cos(angle) / math.sqrt(length)
    sine = np.sin(angle) / math.sqrt(length)
    upper = np.concatenate([cosine, -sine], axis=1)
    lower = np.concatenate([sine, cosine], axis=1)
    return np.concatenate([upper, lower], axis=0).astype(BF16)


def iota(shape, dim):
    return lax.broadcasted_iota(jnp.int32, shape, dim)


def lane_blocks(arrays, width, shift):
    count = len(arrays)
    block = iota(arrays[0].shape, 1) // width
    result = None
    for i, array in enumerate(arrays):
        amount = (i - shift) % count * width
        moved = pltpu.roll(array, amount, 1) if amount else array
        result = moved if result is None else jnp.where(block == i, moved, result)
    return result


def front_kernel(times, blocks, near, beams, volt_any, feed_ref, table_any, out_ref, volt_ref, table_ref, along_ref, sems):
    load = pltpu.make_async_copy(volt_any, volt_ref, sems.at[0])
    load_table = pltpu.make_async_copy(table_any, table_ref, sems.at[1])
    load.start()
    load_table.start()
    rows, feeds = 2 * volt_ref.shape[0], volt_ref.shape[2]
    half = rows // 2
    chans = half // times
    tall = chans // blocks
    i = iota((rows, rows), 0)
    source = i % chans * (2 * times) + i // chans % times * 2 + i // half
    order = jnp.where(iota((rows, rows), 1) == source, 1.0, 0.0).astype(BF16)
    pick = jnp.where(iota((feeds, feeds), 0) == feed_ref[...], 1.0, 0.0).astype(BF16)
    load.wait()
    load_table.wait()
    planes = jnp.dot(order, volt_ref[...].reshape(rows, feeds), preferred_element_type=F32).astype(BF16)
    grid = jnp.dot(planes, pick, preferred_element_type=F32).astype(BF16)
    for gx in range(GX):
        cells = slice(gx * GY, (gx + 1) * GY)
        paired = jnp.concatenate([grid[:half, cells], grid[half:, cells]], axis=1)
        along = jnp.dot(paired, table_ref[...], preferred_element_type=F32)
        along_ref[gx] = along.astype(BF16)
    per_tile = LANES // beams
    group = max(tall, 16)
    for first in range(0, chans, group):
        for tile in range(GY // LANES):
            power = [[] for _ in range(GX)]
            for t in range(times):
                r = pl.ds(t * chans + first, group)
                re = [along_ref[gx, r, pl.ds(tile * LANES, LANES)].astype(F32) for gx in range(GX)]
                im = [along_ref[gx, r, pl.ds(GY + tile * LANES, LANES)].astype(F32) for gx in range(GX)]
                er, ei, orr, oi = re[0] + re[2], im[0] + im[2], re[1] + re[3], im[1] + im[3]
                dr, di, ur, ui = re[0] - re[2], im[0] - im[2], re[1] - re[3], im[1] - im[3]
                formed = [(er + orr, ei + oi), (dr + ui, di - ur), (er - orr, ei - oi), (dr - ui, di + ur)]
                for bx, (fr, fi) in enumerate(formed):
                    fr, fi = 0.5 * fr, 0.5 * fi
                    power[bx].append(0.5 * (fr * fr + fi * fi))
            for bx in range(GX):
                for part in range(per_tile):
                    slab = tile * per_tile + part
                    for u in range(times // per_tile):
                        packed = lane_blocks(power[bx][u * per_tile : (u + 1) * per_tile], beams, part)
                        for row in range(0, group, tall):
                            peer = ((first + row) // tall * near + slab) * GX + bx
                            out_ref[peer, :, pl.ds(u * LANES, LANES)] = packed[row : row + tall].astype(BF16)


def dedisperse_kernel(beams, place_ref, own_any, other_any, lag_any, out_ref, total_ref, own_ref, other_ref, lag_ref, level_ref, sems):
    pairs = ((own_any, own_ref), (other_any, other_ref), (lag_any, lag_ref))
    copies = [pltpu.make_async_copy(a, b, sems.at[i]) for i, (a, b) in enumerate(pairs)]
    for copy in copies:
        copy.start()
    for copy in copies:
        copy.wait()
    sources, tall, width = own_ref.shape
    bands = out_ref.shape[0]
    subs = tall // bands
    chunk = 8
    low = place_ref[0] == 0

    tiles = width // LANES

    def center(i, carry):
        mine = own_ref[pl.ds(i * chunk, chunk)].astype(F32).reshape(chunk * tall, width)
        theirs = other_ref[pl.ds(i * chunk, chunk)].astype(F32).reshape(chunk * tall, width)
        levels = []
        for half in (jnp.where(low, mine, theirs), jnp.where(low, theirs, mine)):
            levels += [half[:, u * LANES : (u + 1) * LANES] for u in range(tiles)]
        total = sum(levels[1:], levels[0])
        amount = LANES // 2
        while amount >= beams:
            total = total + pltpu.roll(total, amount, 1)
            amount //= 2
        mean = total * (0.5 * beams / width)
        r = pl.ds(pl.multiple_of(i * (chunk * tall), chunk * tall), chunk * tall)
        for u, level in enumerate(levels):
            level_ref[u, r, :] = level - mean
        return carry

    lax.fori_loop(0, sources // chunk, center, 0)
    lane = iota((out_ref.shape[1], LANES), 1)
    running = [None] * tiles
    for b in range(bands):
        rows = []
        for s in range(subs):
            r = pl.ds(b * subs + s, sources, stride=tall)
            rows.append(jnp.concatenate([level_ref[u, r, :].astype(BF16) for u in range(2 * tiles)], axis=1))
        data = jnp.concatenate(rows, axis=0)
        lags = lag_ref[lax.rem(b + bands - place_ref[1], bands)].astype(F32)
        for v in range(LAGS):
            chosen = jnp.where(lags == float(v), 1.0, 0.0).astype(BF16)
            picked = jnp.dot(chosen, data, preferred_element_type=F32)
            for u in range(tiles):
                whole, rest = divmod(v * beams + u * LANES, LANES)
                part = picked[:, whole * LANES : (whole + 1) * LANES]
                if rest:
                    after = picked[:, (whole + 1) * LANES : (whole + 2) * LANES]
                    back = LANES - rest
                    part = jnp.where(lane < back, pltpu.roll(part, back, 1), pltpu.roll(after, back, 1))
                running[u] = part if running[u] is None else running[u] + part
        for u in range(tiles):
            out_ref[b, :, pl.ds(u * LANES, LANES)] = running[u]
    for u in range(tiles):
        total_ref[:, pl.ds(u * LANES, LANES)] = running[u]


def spread_kernel(beams, scale, in_any, out_ref, in_ref, sem):
    copy = pltpu.make_async_copy(in_any, in_ref, sem)
    copy.start()
    copy.wait()
    slabs, trials, width = in_ref.shape
    times = width // beams
    count = LANES // beams
    stride = slabs // count * times
    for tile in range(slabs // count):
        for t in range(times):
            source, shift = t * beams // LANES, t * beams % LANES // beams
            cut = pl.ds(source * LANES, LANES)
            parts = [in_ref[tile * count + i, :, cut].astype(F32) * scale for i in range(count)]
            out_ref[pl.ds(tile * times + t, trials, stride=stride), :] = lane_blocks(parts, beams, shift)


def search(voltages, grid_feed, delays):
    bands, sub_local, times = voltages.shape[:3]
    feeds = voltages.shape[4]
    blocks, near, columns = lax.axis_size("far"), lax.axis_size("near"), lax.axis_size("beam")
    peers = blocks * near * columns
    beams = feeds // columns // near
    trials = delays.shape[2]
    subs = delays.shape[1]
    tall = bands // blocks * sub_local
    rows = bands * sub_local * times * 2
    vmem = pl.BlockSpec(memory_space=pltpu.VMEM)
    anywhere = pl.BlockSpec(memory_space=pl.ANY)

    lag_rows = delays[0].astype(BF16).reshape(peers, sub_local, trials)
    lag_rows = jnp.transpose(lag_rows, (2, 1, 0)).reshape(trials, subs)

    sent = pl.pallas_call(
        functools.partial(front_kernel, times, blocks, near, beams),
        out_shape=jax.ShapeDtypeStruct((peers, tall, times * beams), BF16),
        in_specs=[anywhere, vmem, anywhere],
        out_specs=vmem,
        scratch_shapes=[
            pltpu.VMEM((rows // 2, 2, feeds), BF16),
            pltpu.VMEM((2 * GY, 2 * GY), BF16),
            pltpu.VMEM((GX, rows // 2, 2 * GY), BF16),
            pltpu.SemaphoreType.DMA((2,)),
        ],
        cost_estimate=pl.CostEstimate(flops=2 * 10**9, bytes_accessed=4 * 10**6, transcendentals=0),
        name="front",
    )(voltages.reshape(rows // 2, 2, feeds), grid_feed.reshape(1, feeds), jnp.asarray(steering_table(GY)))
    own = lax.all_to_all(sent, ("far", "near", "beam"), split_axis=0, concat_axis=0, tiled=True)
    share = near // columns
    fetched = []
    for j in range(share):
        steps = [(n, x, (n + x * share + j) % near) for n in range(near) for x in range(columns)]
        pairs = [(source * columns + x, n * columns + x) for n, x, source in steps]
        fetched.append(lax.ppermute(lag_rows, ("near", "beam"), pairs))
    lags = lax.all_gather(jnp.stack(fetched), "beam").reshape(near, trials, subs)
    other = lax.ppermute(own, "dm", [(0, 1), (1, 0)])
    place = jnp.stack([lax.axis_index("dm"), lax.axis_index("near")]).astype(jnp.int32)
    local, total = pl.pallas_call(
        functools.partial(dedisperse_kernel, beams),
        out_shape=(
            jax.ShapeDtypeStruct((bands // blocks, trials, times * beams), F32),
            jax.ShapeDtypeStruct((trials, times * beams), F32),
        ),
        in_specs=[pl.BlockSpec(memory_space=pltpu.SMEM)] + [anywhere] * 3,
        out_specs=(vmem, vmem),
        scratch_shapes=[
            pltpu.VMEM(own.shape, BF16),
            pltpu.VMEM(own.shape, BF16),
            pltpu.VMEM(lags.shape, BF16),
            pltpu.VMEM((2 * times * beams // LANES, peers * tall, LANES), F32),
            pltpu.SemaphoreType.DMA((3,)),
        ],
        compiler_params=pltpu.CompilerParams(vmem_limit_bytes=24 * 2**20),
        cost_estimate=pl.CostEstimate(flops=2 * 10**9, bytes_accessed=4 * 10**6, transcendentals=0),
        name="dedisperse",
    )(place, own, other, lags)
    inner = lax.ppermute(total.astype(BF16), "far", [(k, k + 1) for k in range(0, blocks, 2)]).astype(F32)
    through = total + inner
    before = jnp.zeros_like(total)
    for k in range(1, blocks - 2, 2):
        before = before + lax.ppermute((before + through).astype(BF16), "far", [(k, k + 2)]).astype(F32)
    handed = lax.ppermute((before + through).astype(BF16), "far", [(k, k + 1) for k in range(1, blocks - 1, 2)])
    base = inner + before + handed.astype(F32)
    cumulative = (local + base).astype(BF16)
    slabs = lax.all_to_all(cumulative, "near", split_axis=0, concat_axis=0, tiled=True)
    spread = pl.pallas_call(
        functools.partial(spread_kernel, beams, 1.0 / math.sqrt(FREQS)),
        out_shape=jax.ShapeDtypeStruct((trials * times * near * beams // LANES, LANES), F32),
        in_specs=[anywhere],
        out_specs=vmem,
        scratch_shapes=[pltpu.VMEM(slabs.shape, BF16), pltpu.SemaphoreType.DMA],
        compiler_params=pltpu.CompilerParams(vmem_limit_bytes=24 * 2**20),
        name="spread",
    )(slabs)
    spread = jnp.transpose(spread.reshape(trials, near * beams // LANES, times, LANES), (0, 2, 1, 3))
    return spread.reshape(1, trials, times, near * beams)


def solution(mesh):
    near = 4
    sizes = mesh.shape
    devices = mesh.devices.reshape(sizes["grp"], sizes["freq"] // near, near, sizes["beam"], sizes["dm"])
    split = Mesh(devices, ("grp", "far", "near", "beam", "dm"))
    freq = ("far", "near")
    in_specs = (P(None, (*freq, "beam"), ("grp", "dm"), None, None), P(), P(freq, None, "dm"))
    out_specs = P(freq, "dm", "grp", "beam")
    return jax.shard_map(search, mesh=split, in_specs=in_specs, out_specs=out_specs, check_vma=False)
```

```python
import functools
import math

import jax
import jax.numpy as jnp
import numpy as np
from jax import lax
from jax.experimental import pallas as pl
from jax.experimental.pallas import tpu as pltpu
from jax.sharding import Mesh
from jax.sharding import PartitionSpec as P


GX = 4
GY = 256
FREQS = 8192
LAGS = 5
LANES = 128
BF16 = jnp.bfloat16
F32 = jnp.float32


def steering_table(length):
    position = np.arange(length)
    angle = (position[:, None] * position[None, :] % length) * (2.0 * math.pi / length)
    cosine = np.cos(angle) / math.sqrt(length)
    sine = np.sin(angle) / math.sqrt(length)
    upper = np.concatenate([cosine, -sine], axis=1)
    lower = np.concatenate([sine, cosine], axis=1)
    return np.concatenate([upper, lower], axis=0).astype(BF16)


def iota(shape, dim):
    return lax.broadcasted_iota(jnp.int32, shape, dim)


def lane_blocks(arrays, width, shift):
    count = len(arrays)
    block = iota(arrays[0].shape, 1) // width
    result = None
    for i, array in enumerate(arrays):
        amount = (i - shift) % count * width
        moved = pltpu.roll(array, amount, 1) if amount else array
        result = moved if result is None else jnp.where(block == i, moved, result)
    return result


def front_kernel(times, blocks, near, beams, volt_ref, feed_ref, table_ref, out_ref, along_ref):
    rows, feeds = 2 * volt_ref.shape[0], volt_ref.shape[2]
    half = rows // 2
    chans = half // times
    tall = chans // blocks
    i = iota((rows, rows), 0)
    source = i % chans * (2 * times) + i // chans % times * 2 + i // half
    order = jnp.where(iota((rows, rows), 1) == source, 1.0, 0.0).astype(BF16)
    pick = jnp.where(iota((feeds, feeds), 0) == feed_ref[...], 1.0, 0.0).astype(BF16)
    planes = jnp.dot(order, volt_ref[...].reshape(rows, feeds), preferred_element_type=F32).astype(BF16)
    grid = jnp.dot(planes, pick, preferred_element_type=F32).astype(BF16)
    for gx in range(GX):
        cells = slice(gx * GY, (gx + 1) * GY)
        paired = jnp.concatenate([grid[:half, cells], grid[half:, cells]], axis=1)
        along = jnp.dot(paired, table_ref[...], preferred_element_type=F32)
        along_ref[gx] = along.astype(BF16)
    per_tile = LANES // beams
    group = max(tall, 16)
    for first in range(0, chans, group):
        for tile in range(GY // LANES):
            power = [[] for _ in range(GX)]
            for t in range(times):
                r = pl.ds(t * chans + first, group)
                re = [along_ref[gx, r, pl.ds(tile * LANES, LANES)].astype(F32) for gx in range(GX)]
                im = [along_ref[gx, r, pl.ds(GY + tile * LANES, LANES)].astype(F32) for gx in range(GX)]
                er, ei, orr, oi = re[0] + re[2], im[0] + im[2], re[1] + re[3], im[1] + im[3]
                dr, di, ur, ui = re[0] - re[2], im[0] - im[2], re[1] - re[3], im[1] - im[3]
                formed = [(er + orr, ei + oi), (dr + ui, di - ur), (er - orr, ei - oi), (dr - ui, di + ur)]
                for bx, (fr, fi) in enumerate(formed):
                    fr, fi = 0.5 * fr, 0.5 * fi
                    power[bx].append(0.5 * (fr * fr + fi * fi))
            for bx in range(GX):
                for part in range(per_tile):
                    slab = tile * per_tile + part
                    for u in range(times // per_tile):
                        packed = lane_blocks(power[bx][u * per_tile : (u + 1) * per_tile], beams, part)
                        for row in range(0, group, tall):
                            peer = ((first + row) // tall * near + slab) * GX + bx
                            out_ref[peer, :, pl.ds(u * LANES, LANES)] = packed[row : row + tall].astype(BF16)


def dedisperse_kernel(beams, place_ref, own_any, other_any, lag_any, out_ref, total_ref, own_ref, other_ref, lag_ref, level_ref, sems):
    pairs = ((own_any, own_ref), (other_any, other_ref), (lag_any, lag_ref))
    copies = [pltpu.make_async_copy(a, b, sems.at[i]) for i, (a, b) in enumerate(pairs)]
    for copy in copies:
        copy.start()
    for copy in copies:
        copy.wait()
    sources, tall, width = own_ref.shape
    bands = out_ref.shape[0]
    subs = tall // bands
    chunk = 8
    low = place_ref[0] == 0

    tiles = width // LANES

    def center(i, carry):
        mine = own_ref[pl.ds(i * chunk, chunk)].astype(F32).reshape(chunk * tall, width)
        theirs = other_ref[pl.ds(i * chunk, chunk)].astype(F32).reshape(chunk * tall, width)
        levels = []
        for half in (jnp.where(low, mine, theirs), jnp.where(low, theirs, mine)):
            levels += [half[:, u * LANES : (u + 1) * LANES] for u in range(tiles)]
        total = sum(levels[1:], levels[0])
        amount = LANES // 2
        while amount >= beams:
            total = total + pltpu.roll(total, amount, 1)
            amount //= 2
        mean = total * (0.5 * beams / width)
        r = pl.ds(pl.multiple_of(i * (chunk * tall), chunk * tall), chunk * tall)
        for u, level in enumerate(levels):
            level_ref[u, r, :] = level - mean
        return carry

    lax.fori_loop(0, sources // chunk, center, 0)
    lane = iota((out_ref.shape[1], LANES), 1)
    running = [None] * tiles
    for b in range(bands):
        rows = []
        for s in range(subs):
            r = pl.ds(b * subs + s, sources, stride=tall)
            rows.append(jnp.concatenate([level_ref[u, r, :].astype(BF16) for u in range(2 * tiles)], axis=1))
        data = jnp.concatenate(rows, axis=0)
        lags = lag_ref[lax.rem(b + bands - place_ref[1], bands)].astype(F32)
        for v in range(LAGS):
            chosen = jnp.where(lags == float(v), 1.0, 0.0).astype(BF16)
            picked = jnp.dot(chosen, data, preferred_element_type=F32)
            for u in range(tiles):
                whole, rest = divmod(v * beams + u * LANES, LANES)
                part = picked[:, whole * LANES : (whole + 1) * LANES]
                if rest:
                    after = picked[:, (whole + 1) * LANES : (whole + 2) * LANES]
                    back = LANES - rest
                    part = jnp.where(lane < back, pltpu.roll(part, back, 1), pltpu.roll(after, back, 1))
                running[u] = part if running[u] is None else running[u] + part
        for u in range(tiles):
            out_ref[b, :, pl.ds(u * LANES, LANES)] = running[u]
    for u in range(tiles):
        total_ref[:, pl.ds(u * LANES, LANES)] = running[u]


def spread_kernel(beams, scale, in_any, out_ref, in_ref, sem):
    copy = pltpu.make_async_copy(in_any, in_ref, sem)
    copy.start()
    copy.wait()
    slabs, trials, width = in_ref.shape
    times = width // beams
    count = LANES // beams
    stride = slabs // count * times
    for tile in range(slabs // count):
        for t in range(times):
            source, shift = t * beams // LANES, t * beams % LANES // beams
            cut = pl.ds(source * LANES, LANES)
            parts = [in_ref[tile * count + i, :, cut].astype(F32) * scale for i in range(count)]
            out_ref[pl.ds(tile * times + t, trials, stride=stride), :] = lane_blocks(parts, beams, shift)


def search(voltages, grid_feed, delays):
    bands, sub_local, times = voltages.shape[:3]
    feeds = voltages.shape[4]
    blocks, near, columns = lax.axis_size("far"), lax.axis_size("near"), lax.axis_size("beam")
    peers = blocks * near * columns
    beams = feeds // columns // near
    trials = delays.shape[2]
    subs = delays.shape[1]
    tall = bands // blocks * sub_local
    rows = bands * sub_local * times * 2
    vmem = pl.BlockSpec(memory_space=pltpu.VMEM)
    anywhere = pl.BlockSpec(memory_space=pl.ANY)

    sent = pl.pallas_call(
        functools.partial(front_kernel, times, blocks, near, beams),
        out_shape=jax.ShapeDtypeStruct((peers, tall, times * beams), BF16),
        in_specs=[vmem] * 3,
        out_specs=vmem,
        scratch_shapes=[pltpu.VMEM((GX, rows // 2, 2 * GY), BF16)],
        cost_estimate=pl.CostEstimate(flops=2 * 10**9, bytes_accessed=4 * 10**6, transcendentals=0),
        name="front",
    )(voltages.reshape(rows // 2, 2, feeds), grid_feed.reshape(1, feeds), jnp.asarray(steering_table(GY)))
    own = lax.all_to_all(sent, ("far", "near", "beam"), split_axis=0, concat_axis=0, tiled=True)
    share = near // columns
    fetched = []
    for j in range(share):
        steps = [(n, x, (n + x * share + j) % near) for n in range(near) for x in range(columns)]
        pairs = [(source * columns + x, n * columns + x) for n, x, source in steps]
        fetched.append(lax.ppermute(delays, ("near", "beam"), pairs))
    lags = jnp.concatenate(fetched).astype(BF16).reshape(share, peers, sub_local, trials)
    lags = jnp.transpose(lags, (0, 3, 2, 1)).reshape(share, trials, subs)
    lags = lax.all_gather(lags, "beam").reshape(near, trials, subs)
    other = lax.ppermute(own, "dm", [(0, 1), (1, 0)])
    place = jnp.stack([lax.axis_index("dm"), lax.axis_index("near")]).astype(jnp.int32)
    local, total = pl.pallas_call(
        functools.partial(dedisperse_kernel, beams),
        out_shape=(
            jax.ShapeDtypeStruct((bands // blocks, trials, times * beams), F32),
            jax.ShapeDtypeStruct((trials, times * beams), F32),
        ),
        in_specs=[pl.BlockSpec(memory_space=pltpu.SMEM)] + [anywhere] * 3,
        out_specs=(vmem, vmem),
        scratch_shapes=[
            pltpu.VMEM(own.shape, BF16),
            pltpu.VMEM(own.shape, BF16),
            pltpu.VMEM(lags.shape, BF16),
            pltpu.VMEM((2 * times * beams // LANES, peers * tall, LANES), F32),
            pltpu.SemaphoreType.DMA((3,)),
        ],
        compiler_params=pltpu.CompilerParams(vmem_limit_bytes=24 * 2**20),
        cost_estimate=pl.CostEstimate(flops=2 * 10**9, bytes_accessed=4 * 10**6, transcendentals=0),
        name="dedisperse",
    )(place, own, other, lags)
    mine = total.astype(BF16)
    inner = lax.ppermute(mine, "far", [(k, k + 1) for k in range(blocks - 1)]).astype(F32)
    before = lax.ppermute(mine, "far", [(0, 2)]).astype(F32)
    through = total + inner
    for k in range(1, blocks - 2, 2):
        pairs = [(k, k + 2)] if k == 1 else [(k - 1, k + 1), (k, k + 2)]
        before = before + lax.ppermute((before + through).astype(BF16), "far", pairs).astype(F32)
    base = inner + before
    cumulative = (local + base).astype(BF16)
    slabs = lax.all_to_all(cumulative, "near", split_axis=0, concat_axis=0, tiled=True)
    spread = pl.pallas_call(
        functools.partial(spread_kernel, beams, 1.0 / math.sqrt(FREQS)),
        out_shape=jax.ShapeDtypeStruct((trials * times * near * beams // LANES, LANES), F32),
        in_specs=[anywhere],
        out_specs=vmem,
        scratch_shapes=[pltpu.VMEM(slabs.shape, BF16), pltpu.SemaphoreType.DMA],
        compiler_params=pltpu.CompilerParams(vmem_limit_bytes=24 * 2**20),
        name="spread",
    )(slabs)
    spread = jnp.transpose(spread.reshape(trials, near * beams // LANES, times, LANES), (0, 2, 1, 3))
    return spread.reshape(1, trials, times, near * beams)


def solution(mesh):
    near = 4
    sizes = mesh.shape
    devices = mesh.devices.reshape(sizes["grp"], sizes["freq"] // near, near, sizes["beam"], sizes["dm"])
    split = Mesh(devices, ("grp", "far", "near", "beam", "dm"))
    freq = ("far", "near")
    in_specs = (P(None, (*freq, "beam"), ("grp", "dm"), None, None), P(), P(freq, None, "dm"))
    out_specs = P(freq, "dm", "grp", "beam")
    return jax.shard_map(search, mesh=split, in_specs=in_specs, out_specs=out_specs, check_vma=False)
```

```python
import functools
import math

import jax
import jax.numpy as jnp
import numpy as np
from jax import lax
from jax.experimental import pallas as pl
from jax.experimental.pallas import tpu as pltpu
from jax.sharding import Mesh
from jax.sharding import PartitionSpec as P


GX = 4
GY = 256
FREQS = 8192
LAGS = 5
LANES = 128
BF16 = jnp.bfloat16
F32 = jnp.float32


def steering_table(length):
    position = np.arange(length)
    angle = (position[:, None] * position[None, :] % length) * (2.0 * math.pi / length)
    cosine = np.cos(angle) / math.sqrt(length)
    sine = np.sin(angle) / math.sqrt(length)
    upper = np.concatenate([cosine, -sine], axis=1)
    lower = np.concatenate([sine, cosine], axis=1)
    return np.concatenate([upper, lower], axis=0).astype(BF16)


def iota(shape, dim):
    return lax.broadcasted_iota(jnp.int32, shape, dim)


def lane_blocks(arrays, width, shift):
    count = len(arrays)
    block = iota(arrays[0].shape, 1) // width
    result = None
    for i, array in enumerate(arrays):
        amount = (i - shift) % count * width
        moved = pltpu.roll(array, amount, 1) if amount else array
        result = moved if result is None else jnp.where(block == i, moved, result)
    return result


def front_kernel(times, blocks, near, beams, volt_ref, feed_ref, table_ref, out_ref, along_ref):
    rows, feeds = 2 * volt_ref.shape[0], volt_ref.shape[2]
    half = rows // 2
    chans = half // times
    tall = chans // blocks
    i = iota((rows, rows), 0)
    source = i % chans * (2 * times) + i // chans % times * 2 + i // half
    order = jnp.where(iota((rows, rows), 1) == source, 1.0, 0.0).astype(BF16)
    pick = jnp.where(iota((feeds, feeds), 0) == feed_ref[...], 1.0, 0.0).astype(BF16)
    planes = jnp.dot(order, volt_ref[...].reshape(rows, feeds), preferred_element_type=F32).astype(BF16)
    grid = jnp.dot(planes, pick, preferred_element_type=F32).astype(BF16)
    for gx in range(GX):
        cells = slice(gx * GY, (gx + 1) * GY)
        paired = jnp.concatenate([grid[:half, cells], grid[half:, cells]], axis=1)
        along = jnp.dot(paired, table_ref[...], preferred_element_type=F32)
        along_ref[gx] = along.astype(BF16)
    per_tile = LANES // beams
    group = max(tall, 16)
    for first in range(0, chans, group):
        for tile in range(GY // LANES):
            power = [[] for _ in range(GX)]
            for t in range(times):
                r = pl.ds(t * chans + first, group)
                re = [along_ref[gx, r, pl.ds(tile * LANES, LANES)].astype(F32) for gx in range(GX)]
                im = [along_ref[gx, r, pl.ds(GY + tile * LANES, LANES)].astype(F32) for gx in range(GX)]
                er, ei, orr, oi = re[0] + re[2], im[0] + im[2], re[1] + re[3], im[1] + im[3]
                dr, di, ur, ui = re[0] - re[2], im[0] - im[2], re[1] - re[3], im[1] - im[3]
                formed = [(er + orr, ei + oi), (dr + ui, di - ur), (er - orr, ei - oi), (dr - ui, di + ur)]
                for bx, (fr, fi) in enumerate(formed):
                    fr, fi = 0.5 * fr, 0.5 * fi
                    power[bx].append(0.5 * (fr * fr + fi * fi))
            for bx in range(GX):
                for part in range(per_tile):
                    slab = tile * per_tile + part
                    for u in range(times // per_tile):
                        packed = lane_blocks(power[bx][u * per_tile : (u + 1) * per_tile], beams, part)
                        for row in range(0, group, tall):
                            peer = ((first + row) // tall * near + slab) * GX + bx
                            out_ref[peer, :, pl.ds(u * LANES, LANES)] = packed[row : row + tall].astype(BF16)


def dedisperse_kernel(beams, place_ref, own_any, other_any, lag_any, out_ref, total_ref, own_ref, other_ref, lag_ref, level_ref, sems):
    pairs = ((own_any, own_ref), (other_any, other_ref), (lag_any, lag_ref))
    copies = [pltpu.make_async_copy(a, b, sems.at[i]) for i, (a, b) in enumerate(pairs)]
    for copy in copies:
        copy.start()
    for copy in copies:
        copy.wait()
    sources, tall, width = own_ref.shape
    bands = out_ref.shape[0]
    subs = tall // bands
    chunk = 8
    low = place_ref[0] == 0

    tiles = width // LANES

    def center(i, carry):
        mine = own_ref[pl.ds(i * chunk, chunk)].astype(F32).reshape(chunk * tall, width)
        theirs = other_ref[pl.ds(i * chunk, chunk)].astype(F32).reshape(chunk * tall, width)
        levels = []
        for half in (jnp.where(low, mine, theirs), jnp.where(low, theirs, mine)):
            levels += [half[:, u * LANES : (u + 1) * LANES] for u in range(tiles)]
        total = sum(levels[1:], levels[0])
        amount = LANES // 2
        while amount >= beams:
            total = total + pltpu.roll(total, amount, 1)
            amount //= 2
        mean = total * (0.5 * beams / width)
        r = pl.ds(pl.multiple_of(i * (chunk * tall), chunk * tall), chunk * tall)
        for u, level in enumerate(levels):
            level_ref[u, r, :] = level - mean
        return carry

    lax.fori_loop(0, sources // chunk, center, 0)
    lane = iota((out_ref.shape[1], LANES), 1)
    running = [None] * tiles
    for b in range(bands):
        rows = []
        for s in range(subs):
            r = pl.ds(b * subs + s, sources, stride=tall)
            rows.append(jnp.concatenate([level_ref[u, r, :].astype(BF16) for u in range(2 * tiles)], axis=1))
        data = jnp.concatenate(rows, axis=0)
        lags = lag_ref[lax.rem(b + bands - place_ref[1], bands)].astype(F32)
        for v in range(LAGS):
            chosen = jnp.where(lags == float(v), 1.0, 0.0).astype(BF16)
            picked = jnp.dot(chosen, data, preferred_element_type=F32)
            for u in range(tiles):
                whole, rest = divmod(v * beams + u * LANES, LANES)
                part = picked[:, whole * LANES : (whole + 1) * LANES]
                if rest:
                    after = picked[:, (whole + 1) * LANES : (whole + 2) * LANES]
                    back = LANES - rest
                    part = jnp.where(lane < back, pltpu.roll(part, back, 1), pltpu.roll(after, back, 1))
                running[u] = part if running[u] is None else running[u] + part
        for u in range(tiles):
            out_ref[b, :, pl.ds(u * LANES, LANES)] = running[u]
    for u in range(tiles):
        total_ref[:, pl.ds(u * LANES, LANES)] = running[u]


def spread_kernel(beams, scale, in_any, out_ref, in_ref, sem):
    copy = pltpu.make_async_copy(in_any, in_ref, sem)
    copy.start()
    copy.wait()
    slabs, trials, width = in_ref.shape
    times = width // beams
    count = LANES // beams
    stride = slabs // count * times
    for tile in range(slabs // count):
        for t in range(times):
            source, shift = t * beams // LANES, t * beams % LANES // beams
            cut = pl.ds(source * LANES, LANES)
            parts = [in_ref[tile * count + i, :, cut].astype(F32) * scale for i in range(count)]
            out_ref[pl.ds(tile * times + t, trials, stride=stride), :] = lane_blocks(parts, beams, shift)


def search(voltages, grid_feed, delays):
    bands, sub_local, times = voltages.shape[:3]
    feeds = voltages.shape[4]
    blocks, near, columns = lax.axis_size("far"), lax.axis_size("near"), lax.axis_size("beam")
    peers = blocks * near * columns
    beams = feeds // columns // near
    trials = delays.shape[2]
    subs = delays.shape[1]
    tall = bands // blocks * sub_local
    rows = bands * sub_local * times * 2
    vmem = pl.BlockSpec(memory_space=pltpu.VMEM)
    anywhere = pl.BlockSpec(memory_space=pl.ANY)

    sent = pl.pallas_call(
        functools.partial(front_kernel, times, blocks, near, beams),
        out_shape=jax.ShapeDtypeStruct((peers, tall, times * beams), BF16),
        in_specs=[vmem] * 3,
        out_specs=vmem,
        scratch_shapes=[pltpu.VMEM((GX, rows // 2, 2 * GY), BF16)],
        cost_estimate=pl.CostEstimate(flops=2 * 10**9, bytes_accessed=4 * 10**6, transcendentals=0),
        name="front",
    )(voltages.reshape(rows // 2, 2, feeds), grid_feed.reshape(1, feeds), jnp.asarray(steering_table(GY)))
    own = lax.all_to_all(sent, ("far", "near", "beam"), split_axis=0, concat_axis=0, tiled=True)
    share = near // columns
    fetched = []
    for j in range(share):
        steps = [(n, x, (n + x * share + j) % near) for n in range(near) for x in range(columns)]
        pairs = [(source * columns + x, n * columns + x) for n, x, source in steps]
        fetched.append(lax.ppermute(delays, ("near", "beam"), pairs))
    lags = jnp.concatenate(fetched).astype(BF16).reshape(share, peers, sub_local, trials)
    lags = jnp.transpose(lags, (0, 3, 2, 1)).reshape(share, trials, subs)
    lags = lax.all_gather(lags, "beam").reshape(near, trials, subs)
    other = lax.ppermute(own, "dm", [(0, 1), (1, 0)])
    place = jnp.stack([lax.axis_index("dm"), lax.axis_index("near")]).astype(jnp.int32)
    local, total = pl.pallas_call(
        functools.partial(dedisperse_kernel, beams),
        out_shape=(
            jax.ShapeDtypeStruct((bands // blocks, trials, times * beams), F32),
            jax.ShapeDtypeStruct((trials, times * beams), F32),
        ),
        in_specs=[pl.BlockSpec(memory_space=pltpu.SMEM)] + [anywhere] * 3,
        out_specs=(vmem, vmem),
        scratch_shapes=[
            pltpu.VMEM(own.shape, BF16),
            pltpu.VMEM(own.shape, BF16),
            pltpu.VMEM(lags.shape, BF16),
            pltpu.VMEM((2 * times * beams // LANES, peers * tall, LANES), F32),
            pltpu.SemaphoreType.DMA((3,)),
        ],
        compiler_params=pltpu.CompilerParams(vmem_limit_bytes=24 * 2**20),
        cost_estimate=pl.CostEstimate(flops=2 * 10**9, bytes_accessed=4 * 10**6, transcendentals=0),
        name="dedisperse",
    )(place, own, other, lags)
    inner = lax.ppermute(total.astype(BF16), "far", [(k, k + 1) for k in range(0, blocks, 2)]).astype(F32)
    through = total + inner
    known = through.astype(BF16)
    before = lax.ppermute(known, "far", [(1, 3)]).astype(F32)
    handed = lax.ppermute(known, "far", [(1, 2)]).astype(F32)
    for k in range(3, blocks - 2, 2):
        before = before + lax.ppermute((before + through).astype(BF16), "far", [(k, k + 2)]).astype(F32)
    later = lax.ppermute((before + through).astype(BF16), "far", [(k, k + 1) for k in range(3, blocks - 1, 2)])
    base = inner + before + handed + later.astype(F32)
    cumulative = (local + base).astype(BF16)
    slabs = lax.all_to_all(cumulative, "near", split_axis=0, concat_axis=0, tiled=True)
    spread = pl.pallas_call(
        functools.partial(spread_kernel, beams, 1.0 / math.sqrt(FREQS)),
        out_shape=jax.ShapeDtypeStruct((trials * times * near * beams // LANES, LANES), F32),
        in_specs=[anywhere],
        out_specs=vmem,
        scratch_shapes=[pltpu.VMEM(slabs.shape, BF16), pltpu.SemaphoreType.DMA],
        compiler_params=pltpu.CompilerParams(vmem_limit_bytes=24 * 2**20),
        name="spread",
    )(slabs)
    spread = jnp.transpose(spread.reshape(trials, near * beams // LANES, times, LANES), (0, 2, 1, 3))
    return spread.reshape(1, trials, times, near * beams)


def solution(mesh):
    near = 4
    sizes = mesh.shape
    devices = mesh.devices.reshape(sizes["grp"], sizes["freq"] // near, near, sizes["beam"], sizes["dm"])
    split = Mesh(devices, ("grp", "far", "near", "beam", "dm"))
    freq = ("far", "near")
    in_specs = (P(None, (*freq, "beam"), ("grp", "dm"), None, None), P(), P(freq, None, "dm"))
    out_specs = P(freq, "dm", "grp", "beam")
    return jax.shard_map(search, mesh=split, in_specs=in_specs, out_specs=out_specs, check_vma=False)
```

```python
import functools
import math

import jax
import jax.numpy as jnp
import numpy as np
from jax import lax
from jax.experimental import pallas as pl
from jax.experimental.pallas import tpu as pltpu
from jax.sharding import Mesh
from jax.sharding import PartitionSpec as P


GX = 4
GY = 256
FREQS = 8192
LAGS = 5
LANES = 128
BF16 = jnp.bfloat16
F32 = jnp.float32


def steering_table(length):
    position = np.arange(length)
    angle = (position[:, None] * position[None, :] % length) * (2.0 * math.pi / length)
    cosine = np.cos(angle) / math.sqrt(length)
    sine = np.sin(angle) / math.sqrt(length)
    upper = np.concatenate([cosine, -sine], axis=1)
    lower = np.concatenate([sine, cosine], axis=1)
    return np.concatenate([upper, lower], axis=0).astype(BF16)


def iota(shape, dim):
    return lax.broadcasted_iota(jnp.int32, shape, dim)


def lane_blocks(arrays, width, shift):
    count = len(arrays)
    block = iota(arrays[0].shape, 1) // width
    result = None
    for i, array in enumerate(arrays):
        amount = (i - shift) % count * width
        moved = pltpu.roll(array, amount, 1) if amount else array
        result = moved if result is None else jnp.where(block == i, moved, result)
    return result


def front_kernel(times, blocks, near, beams, volt_ref, feed_ref, table_ref, out_ref, along_ref):
    rows, feeds = 2 * volt_ref.shape[0], volt_ref.shape[2]
    half = rows // 2
    chans = half // times
    tall = chans // blocks
    i = iota((rows, rows), 0)
    source = i % chans * (2 * times) + i // chans % times * 2 + i // half
    order = jnp.where(iota((rows, rows), 1) == source, 1.0, 0.0).astype(BF16)
    pick = jnp.where(iota((feeds, feeds), 0) == feed_ref[...], 1.0, 0.0).astype(BF16)
    planes = jnp.dot(order, volt_ref[...].reshape(rows, feeds), preferred_element_type=F32).astype(BF16)
    grid = jnp.dot(planes, pick, preferred_element_type=F32).astype(BF16)
    for gx in range(GX):
        cells = slice(gx * GY, (gx + 1) * GY)
        paired = jnp.concatenate([grid[:half, cells], grid[half:, cells]], axis=1)
        along = jnp.dot(paired, table_ref[...], preferred_element_type=F32)
        along_ref[gx] = along.astype(BF16)
    per_tile = LANES // beams
    group = max(tall, 16)
    for first in range(0, chans, group):
        for tile in range(GY // LANES):
            power = [[] for _ in range(GX)]
            for t in range(times):
                r = pl.ds(t * chans + first, group)
                re = [along_ref[gx, r, pl.ds(tile * LANES, LANES)].astype(F32) for gx in range(GX)]
                im = [along_ref[gx, r, pl.ds(GY + tile * LANES, LANES)].astype(F32) for gx in range(GX)]
                er, ei, orr, oi = re[0] + re[2], im[0] + im[2], re[1] + re[3], im[1] + im[3]
                dr, di, ur, ui = re[0] - re[2], im[0] - im[2], re[1] - re[3], im[1] - im[3]
                formed = [(er + orr, ei + oi), (dr + ui, di - ur), (er - orr, ei - oi), (dr - ui, di + ur)]
                for bx, (fr, fi) in enumerate(formed):
                    fr, fi = 0.5 * fr, 0.5 * fi
                    power[bx].append(0.5 * (fr * fr + fi * fi))
            for bx in range(GX):
                for part in range(per_tile):
                    slab = tile * per_tile + part
                    for u in range(times // per_tile):
                        packed = lane_blocks(power[bx][u * per_tile : (u + 1) * per_tile], beams, part)
                        for row in range(0, group, tall):
                            peer = ((first + row) // tall * near + slab) * GX + bx
                            out_ref[peer, :, pl.ds(u * LANES, LANES)] = packed[row : row + tall].astype(BF16)


def dedisperse_kernel(beams, place_ref, own_any, other_any, lag_any, out_ref, total_ref, own_ref, other_ref, lag_ref, level_ref, sems):
    pairs = ((own_any, own_ref), (other_any, other_ref), (lag_any, lag_ref))
    copies = [pltpu.make_async_copy(a, b, sems.at[i]) for i, (a, b) in enumerate(pairs)]
    for copy in copies:
        copy.start()
    for copy in copies:
        copy.wait()
    sources, tall, width = own_ref.shape
    bands = out_ref.shape[0]
    subs = tall // bands
    chunk = 8
    low = place_ref[0] == 0

    tiles = width // LANES

    def center(i, carry):
        mine = own_ref[pl.ds(i * chunk, chunk)].astype(F32).reshape(chunk * tall, width)
        theirs = other_ref[pl.ds(i * chunk, chunk)].astype(F32).reshape(chunk * tall, width)
        levels = []
        for half in (jnp.where(low, mine, theirs), jnp.where(low, theirs, mine)):
            levels += [half[:, u * LANES : (u + 1) * LANES] for u in range(tiles)]
        total = sum(levels[1:], levels[0])
        amount = LANES // 2
        while amount >= beams:
            total = total + pltpu.roll(total, amount, 1)
            amount //= 2
        mean = total * (0.5 * beams / width)
        r = pl.ds(pl.multiple_of(i * (chunk * tall), chunk * tall), chunk * tall)
        for u, level in enumerate(levels):
            level_ref[u, r, :] = level - mean
        return carry

    lax.fori_loop(0, sources // chunk, center, 0)
    lane = iota((out_ref.shape[1], LANES), 1)
    running = [None] * tiles
    for b in range(bands):
        rows = []
        for s in range(subs):
            r = pl.ds(b * subs + s, sources, stride=tall)
            rows.append(jnp.concatenate([level_ref[u, r, :].astype(BF16) for u in range(2 * tiles)], axis=1))
        data = jnp.concatenate(rows, axis=0)
        lags = lag_ref[lax.rem(b + bands - place_ref[1], bands)].astype(F32)
        for v in range(LAGS):
            chosen = jnp.where(lags == float(v), 1.0, 0.0).astype(BF16)
            picked = jnp.dot(chosen, data, preferred_element_type=F32)
            for u in range(tiles):
                whole, rest = divmod(v * beams + u * LANES, LANES)
                part = picked[:, whole * LANES : (whole + 1) * LANES]
                if rest:
                    after = picked[:, (whole + 1) * LANES : (whole + 2) * LANES]
                    back = LANES - rest
                    part = jnp.where(lane < back, pltpu.roll(part, back, 1), pltpu.roll(after, back, 1))
                running[u] = part if running[u] is None else running[u] + part
        for u in range(tiles):
            out_ref[b, :, pl.ds(u * LANES, LANES)] = running[u]
    for u in range(tiles):
        total_ref[:, pl.ds(u * LANES, LANES)] = running[u]


def spread_kernel(beams, scale, place_ref, *refs):
    pieces, (out_ref, in_ref, sems) = refs[:-3], refs[-3:]
    near = len(pieces)
    copies = []
    for d, piece in enumerate(pieces):
        slab = lax.rem(place_ref[1] + near - d, near)
        copies.append(pltpu.make_async_copy(piece, in_ref.at[slab], sems.at[d]))
    for copy in copies:
        copy.start()
    for copy in copies:
        copy.wait()
    slabs, trials, width = in_ref.shape
    times = width // beams
    count = LANES // beams
    stride = slabs // count * times
    for tile in range(slabs // count):
        for t in range(times):
            source, shift = t * beams // LANES, t * beams % LANES // beams
            cut = pl.ds(source * LANES, LANES)
            parts = [in_ref[tile * count + i, :, cut].astype(F32) * scale for i in range(count)]
            out_ref[pl.ds(tile * times + t, trials, stride=stride), :] = lane_blocks(parts, beams, shift)


def search(voltages, grid_feed, delays):
    bands, sub_local, times = voltages.shape[:3]
    feeds = voltages.shape[4]
    blocks, near, columns = lax.axis_size("far"), lax.axis_size("near"), lax.axis_size("beam")
    peers = blocks * near * columns
    beams = feeds // columns // near
    trials = delays.shape[2]
    subs = delays.shape[1]
    tall = bands // blocks * sub_local
    rows = bands * sub_local * times * 2
    vmem = pl.BlockSpec(memory_space=pltpu.VMEM)
    anywhere = pl.BlockSpec(memory_space=pl.ANY)

    sent = pl.pallas_call(
        functools.partial(front_kernel, times, blocks, near, beams),
        out_shape=jax.ShapeDtypeStruct((peers, tall, times * beams), BF16),
        in_specs=[vmem] * 3,
        out_specs=vmem,
        scratch_shapes=[pltpu.VMEM((GX, rows // 2, 2 * GY), BF16)],
        cost_estimate=pl.CostEstimate(flops=2 * 10**9, bytes_accessed=4 * 10**6, transcendentals=0),
        name="front",
    )(voltages.reshape(rows // 2, 2, feeds), grid_feed.reshape(1, feeds), jnp.asarray(steering_table(GY)))
    own = lax.all_to_all(sent, ("far", "near", "beam"), split_axis=0, concat_axis=0, tiled=True)
    share = near // columns
    fetched = []
    for j in range(share):
        steps = [(n, x, (n + x * share + j) % near) for n in range(near) for x in range(columns)]
        pairs = [(source * columns + x, n * columns + x) for n, x, source in steps]
        fetched.append(lax.ppermute(delays, ("near", "beam"), pairs))
    lags = jnp.concatenate(fetched).astype(BF16).reshape(share, peers, sub_local, trials)
    lags = jnp.transpose(lags, (0, 3, 2, 1)).reshape(share, trials, subs)
    lags = lax.all_gather(lags, "beam").reshape(near, trials, subs)
    other = lax.ppermute(own, "dm", [(0, 1), (1, 0)])
    place = jnp.stack([lax.axis_index("dm"), lax.axis_index("near")]).astype(jnp.int32)
    local, total = pl.pallas_call(
        functools.partial(dedisperse_kernel, beams),
        out_shape=(
            jax.ShapeDtypeStruct((bands // blocks, trials, times * beams), F32),
            jax.ShapeDtypeStruct((trials, times * beams), F32),
        ),
        in_specs=[pl.BlockSpec(memory_space=pltpu.SMEM)] + [anywhere] * 3,
        out_specs=(vmem, vmem),
        scratch_shapes=[
            pltpu.VMEM(own.shape, BF16),
            pltpu.VMEM(own.shape, BF16),
            pltpu.VMEM(lags.shape, BF16),
            pltpu.VMEM((2 * times * beams // LANES, peers * tall, LANES), F32),
            pltpu.SemaphoreType.DMA((3,)),
        ],
        compiler_params=pltpu.CompilerParams(vmem_limit_bytes=24 * 2**20),
        cost_estimate=pl.CostEstimate(flops=2 * 10**9, bytes_accessed=4 * 10**6, transcendentals=0),
        name="dedisperse",
    )(place, own, other, lags)
    inner = lax.ppermute(total.astype(BF16), "far", [(k, k + 1) for k in range(0, blocks, 2)]).astype(F32)
    through = total + inner
    known = through.astype(BF16)
    before = lax.ppermute(known, "far", [(1, 3)]).astype(F32)
    handed = lax.ppermute(known, "far", [(1, 2)]).astype(F32)
    for k in range(3, blocks - 2, 2):
        before = before + lax.ppermute((before + through).astype(BF16), "far", [(k, k + 2)]).astype(F32)
    later = lax.ppermute((before + through).astype(BF16), "far", [(k, k + 1) for k in range(3, blocks - 1, 2)])
    base = inner + before + handed + later.astype(F32)
    pieces = []
    for d in range(near):
        band = lax.rem(lax.axis_index("near") + d, near)
        mine = (lax.dynamic_index_in_dim(local, band, 0, keepdims=False) + base).astype(BF16)
        if d:
            mine = lax.ppermute(mine, "near", [(n, (n + d) % near) for n in range(near)])
        pieces.append(mine)
    spread = pl.pallas_call(
        functools.partial(spread_kernel, beams, 1.0 / math.sqrt(FREQS)),
        out_shape=jax.ShapeDtypeStruct((trials * times * near * beams // LANES, LANES), F32),
        in_specs=[pl.BlockSpec(memory_space=pltpu.SMEM)] + [anywhere] * near,
        out_specs=vmem,
        scratch_shapes=[pltpu.VMEM((near, *base.shape), BF16), pltpu.SemaphoreType.DMA((near,))],
        compiler_params=pltpu.CompilerParams(vmem_limit_bytes=24 * 2**20),
        name="spread",
    )(place, *pieces)
    spread = jnp.transpose(spread.reshape(trials, near * beams // LANES, times, LANES), (0, 2, 1, 3))
    return spread.reshape(1, trials, times, near * beams)


def solution(mesh):
    near = 4
    sizes = mesh.shape
    devices = mesh.devices.reshape(sizes["grp"], sizes["freq"] // near, near, sizes["beam"], sizes["dm"])
    split = Mesh(devices, ("grp", "far", "near", "beam", "dm"))
    freq = ("far", "near")
    in_specs = (P(None, (*freq, "beam"), ("grp", "dm"), None, None), P(), P(freq, None, "dm"))
    out_specs = P(freq, "dm", "grp", "beam")
    return jax.shard_map(search, mesh=split, in_specs=in_specs, out_specs=out_specs, check_vma=False)
```

```python
import functools
import math

import jax
import jax.numpy as jnp
import numpy as np
from jax import lax
from jax.experimental import pallas as pl
from jax.experimental.pallas import tpu as pltpu
from jax.sharding import Mesh
from jax.sharding import PartitionSpec as P


GX = 4
GY = 256
FREQS = 8192
LAGS = 5
LANES = 128
BF16 = jnp.bfloat16
F32 = jnp.float32


def steering_table(length):
    position = np.arange(length)
    angle = (position[:, None] * position[None, :] % length) * (2.0 * math.pi / length)
    cosine = np.cos(angle) / math.sqrt(length)
    sine = np.sin(angle) / math.sqrt(length)
    upper = np.concatenate([cosine, -sine], axis=1)
    lower = np.concatenate([sine, cosine], axis=1)
    return np.concatenate([upper, lower], axis=0).astype(BF16)


def iota(shape, dim):
    return lax.broadcasted_iota(jnp.int32, shape, dim)


def lane_blocks(arrays, width, shift):
    count = len(arrays)
    block = iota(arrays[0].shape, 1) // width
    result = None
    for i, array in enumerate(arrays):
        amount = (i - shift) % count * width
        moved = pltpu.roll(array, amount, 1) if amount else array
        result = moved if result is None else jnp.where(block == i, moved, result)
    return result


def front_kernel(times, blocks, near, beams, volt_ref, feed_ref, table_ref, out_ref, along_ref):
    rows, feeds = 2 * volt_ref.shape[0], volt_ref.shape[2]
    half = rows // 2
    chans = half // times
    tall = chans // blocks
    i = iota((rows, rows), 0)
    source = i % chans * (2 * times) + i // chans % times * 2 + i // half
    order = jnp.where(iota((rows, rows), 1) == source, 1.0, 0.0).astype(BF16)
    pick = jnp.where(iota((feeds, feeds), 0) == feed_ref[...], 1.0, 0.0).astype(BF16)
    planes = jnp.dot(order, volt_ref[...].reshape(rows, feeds), preferred_element_type=F32).astype(BF16)
    grid = jnp.dot(planes, pick, preferred_element_type=F32).astype(BF16)
    for gx in range(GX):
        cells = slice(gx * GY, (gx + 1) * GY)
        paired = jnp.concatenate([grid[:half, cells], grid[half:, cells]], axis=1)
        along = jnp.dot(paired, table_ref[...], preferred_element_type=F32)
        along_ref[gx] = along.astype(BF16)
    per_tile = LANES // beams
    group = max(tall, 16)
    for first in range(0, chans, group):
        for tile in range(GY // LANES):
            power = [[] for _ in range(GX)]
            for t in range(times):
                r = pl.ds(t * chans + first, group)
                re = [along_ref[gx, r, pl.ds(tile * LANES, LANES)].astype(F32) for gx in range(GX)]
                im = [along_ref[gx, r, pl.ds(GY + tile * LANES, LANES)].astype(F32) for gx in range(GX)]
                er, ei, orr, oi = re[0] + re[2], im[0] + im[2], re[1] + re[3], im[1] + im[3]
                dr, di, ur, ui = re[0] - re[2], im[0] - im[2], re[1] - re[3], im[1] - im[3]
                formed = [(er + orr, ei + oi), (dr + ui, di - ur), (er - orr, ei - oi), (dr - ui, di + ur)]
                for bx, (fr, fi) in enumerate(formed):
                    fr, fi = 0.5 * fr, 0.5 * fi
                    power[bx].append(0.5 * (fr * fr + fi * fi))
            for bx in range(GX):
                for part in range(per_tile):
                    slab = tile * per_tile + part
                    for u in range(times // per_tile):
                        packed = lane_blocks(power[bx][u * per_tile : (u + 1) * per_tile], beams, part)
                        for row in range(0, group, tall):
                            peer = ((first + row) // tall * near + slab) * GX + bx
                            out_ref[peer, :, pl.ds(u * LANES, LANES)] = packed[row : row + tall].astype(BF16)


def dedisperse_kernel(beams, turn, place_ref, own_any, other_any, lag_any, *refs):
    earlier, (out_ref, total_ref, *scratch) = refs[:-7], refs[-7:]
    active = lax.rem(place_ref[2], 2) == turn

    @pl.when(active)
    def work():
        dedisperse(beams, place_ref, own_any, other_any, lag_any, out_ref, total_ref, *scratch)

    @pl.when(jnp.logical_not(active))
    def pass_on():
        if not earlier:
            out_ref[...] = jnp.zeros_like(out_ref)
            total_ref[...] = jnp.zeros_like(total_ref)
        else:
            sems = scratch[-1]
            kept = [pltpu.make_async_copy(a, b, sems.at[i]) for i, (a, b) in enumerate(zip(earlier, (out_ref, total_ref)))]
            for copy in kept:
                copy.start()
            for copy in kept:
                copy.wait()


def dedisperse(beams, place_ref, own_any, other_any, lag_any, out_ref, total_ref, own_ref, other_ref, lag_ref, level_ref, sems):
    pairs = ((own_any, own_ref), (other_any, other_ref), (lag_any, lag_ref))
    copies = [pltpu.make_async_copy(a, b, sems.at[i]) for i, (a, b) in enumerate(pairs)]
    for copy in copies:
        copy.start()
    for copy in copies:
        copy.wait()
    sources, tall, width = own_ref.shape
    bands = out_ref.shape[0]
    subs = tall // bands
    chunk = 8
    low = place_ref[0] == 0

    tiles = width // LANES

    def center(i, carry):
        mine = own_ref[pl.ds(i * chunk, chunk)].astype(F32).reshape(chunk * tall, width)
        theirs = other_ref[pl.ds(i * chunk, chunk)].astype(F32).reshape(chunk * tall, width)
        levels = []
        for half in (jnp.where(low, mine, theirs), jnp.where(low, theirs, mine)):
            levels += [half[:, u * LANES : (u + 1) * LANES] for u in range(tiles)]
        total = sum(levels[1:], levels[0])
        amount = LANES // 2
        while amount >= beams:
            total = total + pltpu.roll(total, amount, 1)
            amount //= 2
        mean = total * (0.5 * beams / width)
        r = pl.ds(pl.multiple_of(i * (chunk * tall), chunk * tall), chunk * tall)
        for u, level in enumerate(levels):
            level_ref[u, r, :] = level - mean
        return carry

    lax.fori_loop(0, sources // chunk, center, 0)
    lane = iota((out_ref.shape[1], LANES), 1)
    running = [None] * tiles
    for b in range(bands):
        rows = []
        for s in range(subs):
            r = pl.ds(b * subs + s, sources, stride=tall)
            rows.append(jnp.concatenate([level_ref[u, r, :].astype(BF16) for u in range(2 * tiles)], axis=1))
        data = jnp.concatenate(rows, axis=0)
        lags = lag_ref[lax.rem(b + bands - place_ref[1], bands)].astype(F32)
        for v in range(LAGS):
            chosen = jnp.where(lags == float(v), 1.0, 0.0).astype(BF16)
            picked = jnp.dot(chosen, data, preferred_element_type=F32)
            for u in range(tiles):
                whole, rest = divmod(v * beams + u * LANES, LANES)
                part = picked[:, whole * LANES : (whole + 1) * LANES]
                if rest:
                    after = picked[:, (whole + 1) * LANES : (whole + 2) * LANES]
                    back = LANES - rest
                    part = jnp.where(lane < back, pltpu.roll(part, back, 1), pltpu.roll(after, back, 1))
                running[u] = part if running[u] is None else running[u] + part
        for u in range(tiles):
            out_ref[b, :, pl.ds(u * LANES, LANES)] = running[u]
    for u in range(tiles):
        total_ref[:, pl.ds(u * LANES, LANES)] = running[u]


def spread_kernel(beams, scale, in_any, out_ref, in_ref, sem):
    copy = pltpu.make_async_copy(in_any, in_ref, sem)
    copy.start()
    copy.wait()
    slabs, trials, width = in_ref.shape
    times = width // beams
    count = LANES // beams
    stride = slabs // count * times
    for tile in range(slabs // count):
        for t in range(times):
            source, shift = t * beams // LANES, t * beams % LANES // beams
            cut = pl.ds(source * LANES, LANES)
            parts = [in_ref[tile * count + i, :, cut].astype(F32) * scale for i in range(count)]
            out_ref[pl.ds(tile * times + t, trials, stride=stride), :] = lane_blocks(parts, beams, shift)


def search(voltages, grid_feed, delays):
    bands, sub_local, times = voltages.shape[:3]
    feeds = voltages.shape[4]
    blocks, near, columns = lax.axis_size("far"), lax.axis_size("near"), lax.axis_size("beam")
    peers = blocks * near * columns
    beams = feeds // columns // near
    trials = delays.shape[2]
    subs = delays.shape[1]
    tall = bands // blocks * sub_local
    rows = bands * sub_local * times * 2
    vmem = pl.BlockSpec(memory_space=pltpu.VMEM)
    anywhere = pl.BlockSpec(memory_space=pl.ANY)

    sent = pl.pallas_call(
        functools.partial(front_kernel, times, blocks, near, beams),
        out_shape=jax.ShapeDtypeStruct((peers, tall, times * beams), BF16),
        in_specs=[vmem] * 3,
        out_specs=vmem,
        scratch_shapes=[pltpu.VMEM((GX, rows // 2, 2 * GY), BF16)],
        cost_estimate=pl.CostEstimate(flops=2 * 10**9, bytes_accessed=4 * 10**6, transcendentals=0),
        name="front",
    )(voltages.reshape(rows // 2, 2, feeds), grid_feed.reshape(1, feeds), jnp.asarray(steering_table(GY)))
    own = lax.all_to_all(sent, ("far", "near", "beam"), split_axis=0, concat_axis=0, tiled=True)
    share = near // columns
    fetched = []
    for j in range(share):
        steps = [(n, x, (n + x * share + j) % near) for n in range(near) for x in range(columns)]
        pairs = [(source * columns + x, n * columns + x) for n, x, source in steps]
        fetched.append(lax.ppermute(delays, ("near", "beam"), pairs))
    lags = jnp.concatenate(fetched).astype(BF16).reshape(share, peers, sub_local, trials)
    lags = jnp.transpose(lags, (0, 3, 2, 1)).reshape(share, trials, subs)
    lags = lax.all_gather(lags, "beam").reshape(near, trials, subs)
    other = lax.ppermute(own, "dm", [(0, 1), (1, 0)])
    place = jnp.stack([lax.axis_index(name) for name in ("dm", "near", "far")]).astype(jnp.int32)

    def dedispersed(turn, *earlier):
        return pl.pallas_call(
            functools.partial(dedisperse_kernel, beams, turn),
            out_shape=(
                jax.ShapeDtypeStruct((bands // blocks, trials, times * beams), F32),
                jax.ShapeDtypeStruct((trials, times * beams), F32),
            ),
            in_specs=[pl.BlockSpec(memory_space=pltpu.SMEM)] + [anywhere] * (3 + len(earlier)),
            out_specs=(vmem, vmem),
            scratch_shapes=[
                pltpu.VMEM(own.shape, BF16),
                pltpu.VMEM(own.shape, BF16),
                pltpu.VMEM(lags.shape, BF16),
                pltpu.VMEM((2 * times * beams // LANES, peers * tall, LANES), F32),
                pltpu.SemaphoreType.DMA((3,)),
            ],
            compiler_params=pltpu.CompilerParams(vmem_limit_bytes=24 * 2**20),
            cost_estimate=pl.CostEstimate(flops=10**9, bytes_accessed=4 * 10**6, transcendentals=0),
            name="dedisperse",
        )(place, own, other, lags, *earlier)

    local, total = dedispersed(0)
    inner = lax.ppermute(total.astype(BF16), "far", [(k, k + 1) for k in range(0, blocks, 2)]).astype(F32)
    local, total = dedispersed(1, local, total)
    through = total + inner
    known = through.astype(BF16)
    before = lax.ppermute(known, "far", [(1, 3)]).astype(F32)
    handed = lax.ppermute(known, "far", [(1, 2)]).astype(F32)
    for k in range(3, blocks - 2, 2):
        before = before + lax.ppermute((before + through).astype(BF16), "far", [(k, k + 2)]).astype(F32)
    later = lax.ppermute((before + through).astype(BF16), "far", [(k, k + 1) for k in range(3, blocks - 1, 2)])
    base = inner + before + handed + later.astype(F32)
    cumulative = (local + base).astype(BF16)
    slabs = lax.all_to_all(cumulative, "near", split_axis=0, concat_axis=0, tiled=True)
    spread = pl.pallas_call(
        functools.partial(spread_kernel, beams, 1.0 / math.sqrt(FREQS)),
        out_shape=jax.ShapeDtypeStruct((trials * times * near * beams // LANES, LANES), F32),
        in_specs=[anywhere],
        out_specs=vmem,
        scratch_shapes=[pltpu.VMEM(slabs.shape, BF16), pltpu.SemaphoreType.DMA],
        compiler_params=pltpu.CompilerParams(vmem_limit_bytes=24 * 2**20),
        name="spread",
    )(slabs)
    spread = jnp.transpose(spread.reshape(trials, near * beams // LANES, times, LANES), (0, 2, 1, 3))
    return spread.reshape(1, trials, times, near * beams)


def solution(mesh):
    near = 4
    sizes = mesh.shape
    devices = mesh.devices.reshape(sizes["grp"], sizes["freq"] // near, near, sizes["beam"], sizes["dm"])
    split = Mesh(devices, ("grp", "far", "near", "beam", "dm"))
    freq = ("far", "near")
    in_specs = (P(None, (*freq, "beam"), ("grp", "dm"), None, None), P(), P(freq, None, "dm"))
    out_specs = P(freq, "dm", "grp", "beam")
    return jax.shard_map(search, mesh=split, in_specs=in_specs, out_specs=out_specs, check_vma=False)
```

```python
import functools
import math

import jax
import jax.numpy as jnp
import numpy as np
from jax import lax
from jax.experimental import pallas as pl
from jax.experimental.pallas import tpu as pltpu
from jax.sharding import Mesh
from jax.sharding import PartitionSpec as P


GX = 4
GY = 256
FREQS = 8192
LAGS = 5
LANES = 128
BF16 = jnp.bfloat16
F32 = jnp.float32


def steering_table(length):
    position = np.arange(length)
    angle = (position[:, None] * position[None, :] % length) * (2.0 * math.pi / length)
    cosine = np.cos(angle) / math.sqrt(length)
    sine = np.sin(angle) / math.sqrt(length)
    upper = np.concatenate([cosine, -sine], axis=1)
    lower = np.concatenate([sine, cosine], axis=1)
    return np.concatenate([upper, lower], axis=0).astype(BF16)


def iota(shape, dim):
    return lax.broadcasted_iota(jnp.int32, shape, dim)


def lane_blocks(arrays, width, shift):
    count = len(arrays)
    block = iota(arrays[0].shape, 1) // width
    result = None
    for i, array in enumerate(arrays):
        amount = (i - shift) % count * width
        moved = pltpu.roll(array, amount, 1) if amount else array
        result = moved if result is None else jnp.where(block == i, moved, result)
    return result


def front_kernel(times, blocks, near, beams, volt_ref, feed_ref, table_ref, out_ref, along_ref):
    rows, feeds = 2 * volt_ref.shape[0], volt_ref.shape[2]
    chans = rows // (2 * times)
    tall = chans // blocks
    pick = jnp.where(iota((feeds, feeds), 0) == feed_ref[...], 1.0, 0.0).astype(BF16)
    volts = volt_ref[...].reshape(rows, feeds)
    grid = jnp.dot(volts, pick, preferred_element_type=F32).astype(BF16)
    table = table_ref[pl.ds(GY, GY), :]
    halves = GY // LANES
    for gx in range(GX):
        along = jnp.dot(grid[:, gx * GY : (gx + 1) * GY], table, preferred_element_type=F32)
        for u in range(2 * halves):
            along_ref[gx, u] = along[:, u * LANES : (u + 1) * LANES]
    per_tile = LANES // beams
    group = max(tall, 16)
    for first in range(0, chans, group):
        for tile in range(GY // LANES):
            power = [[] for _ in range(GX)]
            for t in range(times):
                r0, r1 = (pl.ds((first * times + t) * 2 + p, group, stride=2 * times) for p in range(2))
                re, im = [], []
                for gx in range(GX):
                    sine, cosine = along_ref.at[gx, tile], along_ref.at[gx, halves + tile]
                    re.append((cosine[r0, :] + sine[r1, :]).astype(BF16).astype(F32))
                    im.append((cosine[r1, :] - sine[r0, :]).astype(BF16).astype(F32))
                er, ei, orr, oi = re[0] + re[2], im[0] + im[2], re[1] + re[3], im[1] + im[3]
                dr, di, ur, ui = re[0] - re[2], im[0] - im[2], re[1] - re[3], im[1] - im[3]
                formed = [(er + orr, ei + oi), (dr + ui, di - ur), (er - orr, ei - oi), (dr - ui, di + ur)]
                for bx, (fr, fi) in enumerate(formed):
                    fr, fi = 0.5 * fr, 0.5 * fi
                    power[bx].append(0.5 * (fr * fr + fi * fi))
            for bx in range(GX):
                for part in range(per_tile):
                    slab = tile * per_tile + part
                    for u in range(times // per_tile):
                        packed = lane_blocks(power[bx][u * per_tile : (u + 1) * per_tile], beams, part)
                        for row in range(0, group, tall):
                            peer = ((first + row) // tall * near + slab) * GX + bx
                            out_ref[peer, :, pl.ds(u * LANES, LANES)] = packed[row : row + tall].astype(BF16)


def dedisperse_kernel(beams, place_ref, own_any, other_any, lag_any, out_ref, total_ref, own_ref, other_ref, lag_ref, level_ref, sems):
    pairs = ((own_any, own_ref), (other_any, other_ref), (lag_any, lag_ref))
    copies = [pltpu.make_async_copy(a, b, sems.at[i]) for i, (a, b) in enumerate(pairs)]
    for copy in copies:
        copy.start()
    for copy in copies:
        copy.wait()
    sources, tall, width = own_ref.shape
    bands = out_ref.shape[0]
    subs = tall // bands
    chunk = 8
    low = place_ref[0] == 0

    tiles = width // LANES

    def center(i, carry):
        mine = own_ref[pl.ds(i * chunk, chunk)].astype(F32).reshape(chunk * tall, width)
        theirs = other_ref[pl.ds(i * chunk, chunk)].astype(F32).reshape(chunk * tall, width)
        levels = []
        for half in (jnp.where(low, mine, theirs), jnp.where(low, theirs, mine)):
            levels += [half[:, u * LANES : (u + 1) * LANES] for u in range(tiles)]
        total = sum(levels[1:], levels[0])
        amount = LANES // 2
        while amount >= beams:
            total = total + pltpu.roll(total, amount, 1)
            amount //= 2
        mean = total * (0.5 * beams / width)
        r = pl.ds(pl.multiple_of(i * (chunk * tall), chunk * tall), chunk * tall)
        for u, level in enumerate(levels):
            level_ref[u, r, :] = level - mean
        return carry

    lax.fori_loop(0, sources // chunk, center, 0)
    lane = iota((out_ref.shape[1], LANES), 1)
    running = [None] * tiles
    for b in range(bands):
        rows = []
        for s in range(subs):
            r = pl.ds(b * subs + s, sources, stride=tall)
            rows.append(jnp.concatenate([level_ref[u, r, :].astype(BF16) for u in range(2 * tiles)], axis=1))
        data = jnp.concatenate(rows, axis=0)
        lags = lag_ref[lax.rem(b + bands - place_ref[1], bands)].astype(F32)
        for v in range(LAGS):
            chosen = jnp.where(lags == float(v), 1.0, 0.0).astype(BF16)
            picked = jnp.dot(chosen, data, preferred_element_type=F32)
            for u in range(tiles):
                whole, rest = divmod(v * beams + u * LANES, LANES)
                part = picked[:, whole * LANES : (whole + 1) * LANES]
                if rest:
                    after = picked[:, (whole + 1) * LANES : (whole + 2) * LANES]
                    back = LANES - rest
                    part = jnp.where(lane < back, pltpu.roll(part, back, 1), pltpu.roll(after, back, 1))
                running[u] = part if running[u] is None else running[u] + part
        for u in range(tiles):
            out_ref[b, :, pl.ds(u * LANES, LANES)] = running[u]
    for u in range(tiles):
        total_ref[:, pl.ds(u * LANES, LANES)] = running[u]


def spread_kernel(beams, scale, in_any, out_ref, in_ref, sem):
    copy = pltpu.make_async_copy(in_any, in_ref, sem)
    copy.start()
    copy.wait()
    slabs, trials, width = in_ref.shape
    times = width // beams
    count = LANES // beams
    stride = slabs // count * times
    for tile in range(slabs // count):
        for t in range(times):
            source, shift = t * beams // LANES, t * beams % LANES // beams
            cut = pl.ds(source * LANES, LANES)
            parts = [in_ref[tile * count + i, :, cut].astype(F32) * scale for i in range(count)]
            out_ref[pl.ds(tile * times + t, trials, stride=stride), :] = lane_blocks(parts, beams, shift)


def search(voltages, grid_feed, delays):
    bands, sub_local, times = voltages.shape[:3]
    feeds = voltages.shape[4]
    blocks, near, columns = lax.axis_size("far"), lax.axis_size("near"), lax.axis_size("beam")
    peers = blocks * near * columns
    beams = feeds // columns // near
    trials = delays.shape[2]
    subs = delays.shape[1]
    tall = bands // blocks * sub_local
    rows = bands * sub_local * times * 2
    vmem = pl.BlockSpec(memory_space=pltpu.VMEM)
    anywhere = pl.BlockSpec(memory_space=pl.ANY)

    sent = pl.pallas_call(
        functools.partial(front_kernel, times, blocks, near, beams),
        out_shape=jax.ShapeDtypeStruct((peers, tall, times * beams), BF16),
        in_specs=[vmem] * 3,
        out_specs=vmem,
        scratch_shapes=[pltpu.VMEM((GX, 2 * GY // LANES, rows, LANES), F32)],
        cost_estimate=pl.CostEstimate(flops=2 * 10**9, bytes_accessed=4 * 10**6, transcendentals=0),
        name="front",
    )(voltages.reshape(rows // 2, 2, feeds), grid_feed.reshape(1, feeds), jnp.asarray(steering_table(GY)))
    own = lax.all_to_all(sent, ("far", "near", "beam"), split_axis=0, concat_axis=0, tiled=True)
    share = near // columns
    fetched = []
    for j in range(share):
        steps = [(n, x, (n + x * share + j) % near) for n in range(near) for x in range(columns)]
        pairs = [(source * columns + x, n * columns + x) for n, x, source in steps]
        fetched.append(lax.ppermute(delays, ("near", "beam"), pairs))
    lags = jnp.concatenate(fetched).astype(BF16).reshape(share, peers, sub_local, trials)
    lags = jnp.transpose(lags, (0, 3, 2, 1)).reshape(share, trials, subs)
    lags = lax.all_gather(lags, "beam").reshape(near, trials, subs)
    other = lax.ppermute(own, "dm", [(0, 1), (1, 0)])
    place = jnp.stack([lax.axis_index("dm"), lax.axis_index("near")]).astype(jnp.int32)
    local, total = pl.pallas_call(
        functools.partial(dedisperse_kernel, beams),
        out_shape=(
            jax.ShapeDtypeStruct((bands // blocks, trials, times * beams), F32),
            jax.ShapeDtypeStruct((trials, times * beams), F32),
        ),
        in_specs=[pl.BlockSpec(memory_space=pltpu.SMEM)] + [anywhere] * 3,
        out_specs=(vmem, vmem),
        scratch_shapes=[
            pltpu.VMEM(own.shape, BF16),
            pltpu.VMEM(own.shape, BF16),
            pltpu.VMEM(lags.shape, BF16),
            pltpu.VMEM((2 * times * beams // LANES, peers * tall, LANES), F32),
            pltpu.SemaphoreType.DMA((3,)),
        ],
        compiler_params=pltpu.CompilerParams(vmem_limit_bytes=24 * 2**20),
        cost_estimate=pl.CostEstimate(flops=2 * 10**9, bytes_accessed=4 * 10**6, transcendentals=0),
        name="dedisperse",
    )(place, own, other, lags)
    inner = lax.ppermute(total.astype(BF16), "far", [(k, k + 1) for k in range(0, blocks, 2)]).astype(F32)
    through = total + inner
    known = through.astype(BF16)
    before = lax.ppermute(known, "far", [(1, 3)]).astype(F32)
    handed = lax.ppermute(known, "far", [(1, 2)]).astype(F32)
    for k in range(3, blocks - 2, 2):
        before = before + lax.ppermute((before + through).astype(BF16), "far", [(k, k + 2)]).astype(F32)
    later = lax.ppermute((before + through).astype(BF16), "far", [(k, k + 1) for k in range(3, blocks - 1, 2)])
    base = inner + before + handed + later.astype(F32)
    cumulative = (local + base).astype(BF16)
    slabs = lax.all_to_all(cumulative, "near", split_axis=0, concat_axis=0, tiled=True)
    spread = pl.pallas_call(
        functools.partial(spread_kernel, beams, 1.0 / math.sqrt(FREQS)),
        out_shape=jax.ShapeDtypeStruct((trials * times * near * beams // LANES, LANES), F32),
        in_specs=[anywhere],
        out_specs=vmem,
        scratch_shapes=[pltpu.VMEM(slabs.shape, BF16), pltpu.SemaphoreType.DMA],
        compiler_params=pltpu.CompilerParams(vmem_limit_bytes=24 * 2**20),
        name="spread",
    )(slabs)
    spread = jnp.transpose(spread.reshape(trials, near * beams // LANES, times, LANES), (0, 2, 1, 3))
    return spread.reshape(1, trials, times, near * beams)


def solution(mesh):
    near = 4
    sizes = mesh.shape
    devices = mesh.devices.reshape(sizes["grp"], sizes["freq"] // near, near, sizes["beam"], sizes["dm"])
    split = Mesh(devices, ("grp", "far", "near", "beam", "dm"))
    freq = ("far", "near")
    in_specs = (P(None, (*freq, "beam"), ("grp", "dm"), None, None), P(), P(freq, None, "dm"))
    out_specs = P(freq, "dm", "grp", "beam")
    return jax.shard_map(search, mesh=split, in_specs=in_specs, out_specs=out_specs, check_vma=False)
```

```python
import functools
import math

import jax
import jax.numpy as jnp
import numpy as np
from jax import lax
from jax.experimental import pallas as pl
from jax.experimental.pallas import tpu as pltpu
from jax.sharding import Mesh
from jax.sharding import PartitionSpec as P


GX = 4
GY = 256
FREQS = 8192
LAGS = 5
LANES = 128
BF16 = jnp.bfloat16
F32 = jnp.float32


def steering_table(length):
    position = np.arange(length)
    angle = (position[:, None] * position[None, :] % length) * (2.0 * math.pi / length)
    cosine = np.cos(angle) / math.sqrt(length)
    sine = np.sin(angle) / math.sqrt(length)
    upper = np.concatenate([cosine, -sine], axis=1)
    lower = np.concatenate([sine, cosine], axis=1)
    return np.concatenate([upper, lower], axis=0).astype(BF16)


def iota(shape, dim):
    return lax.broadcasted_iota(jnp.int32, shape, dim)


def lane_blocks(arrays, width, shift):
    count = len(arrays)
    block = iota(arrays[0].shape, 1) // width
    result = None
    for i, array in enumerate(arrays):
        amount = (i - shift) % count * width
        moved = pltpu.roll(array, amount, 1) if amount else array
        result = moved if result is None else jnp.where(block == i, moved, result)
    return result


def front_kernel(times, blocks, near, beams, volt_ref, feed_ref, table_ref, out_ref, along_ref):
    rows, feeds = 2 * volt_ref.shape[0], volt_ref.shape[2]
    chans = rows // (2 * times)
    tall = chans // blocks
    pick = jnp.where(iota((feeds, feeds), 0) == feed_ref[...], 1.0, 0.0).astype(BF16)
    volts = volt_ref[...].reshape(rows, feeds)
    grid = jnp.dot(volts, pick, preferred_element_type=F32).astype(BF16)
    table = table_ref[pl.ds(GY, GY), :]
    halves = GY // LANES
    for gx in range(GX):
        along = jnp.dot(grid[:, gx * GY : (gx + 1) * GY], table, preferred_element_type=F32)
        for u in range(2 * halves):
            along_ref[gx, u] = along[:, u * LANES : (u + 1) * LANES]
    per_tile = LANES // beams
    group = max(tall, 16)
    for first in range(0, chans, group):
        for tile in range(GY // LANES):
            power = [[] for _ in range(GX)]
            for t in range(times):
                r0, r1 = (pl.ds((first * times + t) * 2 + p, group, stride=2 * times) for p in range(2))
                re, im = [], []
                for gx in range(GX):
                    sine, cosine = along_ref.at[gx, tile], along_ref.at[gx, halves + tile]
                    re.append((cosine[r0, :] + sine[r1, :]).astype(BF16).astype(F32))
                    im.append((cosine[r1, :] - sine[r0, :]).astype(BF16).astype(F32))
                er, ei, orr, oi = re[0] + re[2], im[0] + im[2], re[1] + re[3], im[1] + im[3]
                dr, di, ur, ui = re[0] - re[2], im[0] - im[2], re[1] - re[3], im[1] - im[3]
                formed = [(er + orr, ei + oi), (dr + ui, di - ur), (er - orr, ei - oi), (dr - ui, di + ur)]
                for bx, (fr, fi) in enumerate(formed):
                    fr, fi = 0.5 * fr, 0.5 * fi
                    power[bx].append(0.5 * (fr * fr + fi * fi))
            for bx in range(GX):
                for part in range(per_tile):
                    slab = tile * per_tile + part
                    for u in range(times // per_tile):
                        packed = lane_blocks(power[bx][u * per_tile : (u + 1) * per_tile], beams, part)
                        for row in range(0, group, tall):
                            peer = ((first + row) // tall * near + slab) * GX + bx
                            out_ref[peer, :, pl.ds(u * LANES, LANES)] = packed[row : row + tall].astype(BF16)


def dedisperse_kernel(beams, place_ref, own_ref, other_ref, lag_ref, out_ref, total_ref, level_ref):
    sources, tall, width = own_ref.shape
    bands = out_ref.shape[0]
    subs = tall // bands
    chunk = 8
    low = place_ref[0] == 0

    tiles = width // LANES

    def center(i, carry):
        mine = own_ref[pl.ds(i * chunk, chunk)].astype(F32).reshape(chunk * tall, width)
        theirs = other_ref[pl.ds(i * chunk, chunk)].astype(F32).reshape(chunk * tall, width)
        levels = []
        for half in (jnp.where(low, mine, theirs), jnp.where(low, theirs, mine)):
            levels += [half[:, u * LANES : (u + 1) * LANES] for u in range(tiles)]
        total = sum(levels[1:], levels[0])
        amount = LANES // 2
        while amount >= beams:
            total = total + pltpu.roll(total, amount, 1)
            amount //= 2
        mean = total * (0.5 * beams / width)
        r = pl.ds(pl.multiple_of(i * (chunk * tall), chunk * tall), chunk * tall)
        for u, level in enumerate(levels):
            level_ref[u, r, :] = level - mean
        return carry

    lax.fori_loop(0, sources // chunk, center, 0)
    lane = iota((out_ref.shape[1], LANES), 1)
    running = [None] * tiles
    for b in range(bands):
        rows = []
        for s in range(subs):
            r = pl.ds(b * subs + s, sources, stride=tall)
            rows.append(jnp.concatenate([level_ref[u, r, :].astype(BF16) for u in range(2 * tiles)], axis=1))
        data = jnp.concatenate(rows, axis=0)
        lags = lag_ref[lax.rem(b + bands - place_ref[1], bands)].astype(F32)
        for v in range(LAGS):
            chosen = jnp.where(lags == float(v), 1.0, 0.0).astype(BF16)
            picked = jnp.dot(chosen, data, preferred_element_type=F32)
            for u in range(tiles):
                whole, rest = divmod(v * beams + u * LANES, LANES)
                part = picked[:, whole * LANES : (whole + 1) * LANES]
                if rest:
                    after = picked[:, (whole + 1) * LANES : (whole + 2) * LANES]
                    back = LANES - rest
                    part = jnp.where(lane < back, pltpu.roll(part, back, 1), pltpu.roll(after, back, 1))
                running[u] = part if running[u] is None else running[u] + part
        for u in range(tiles):
            out_ref[b, :, pl.ds(u * LANES, LANES)] = running[u]
    for u in range(tiles):
        total_ref[:, pl.ds(u * LANES, LANES)] = running[u]


def spread_kernel(beams, scale, in_ref, out_ref):
    slabs, trials, width = in_ref.shape
    times = width // beams
    count = LANES // beams
    stride = slabs // count * times
    for tile in range(slabs // count):
        for t in range(times):
            source, shift = t * beams // LANES, t * beams % LANES // beams
            cut = pl.ds(source * LANES, LANES)
            parts = [in_ref[tile * count + i, :, cut].astype(F32) * scale for i in range(count)]
            out_ref[pl.ds(tile * times + t, trials, stride=stride), :] = lane_blocks(parts, beams, shift)


def search(voltages, grid_feed, delays):
    bands, sub_local, times = voltages.shape[:3]
    feeds = voltages.shape[4]
    blocks, near, columns = lax.axis_size("far"), lax.axis_size("near"), lax.axis_size("beam")
    peers = blocks * near * columns
    beams = feeds // columns // near
    trials = delays.shape[2]
    subs = delays.shape[1]
    tall = bands // blocks * sub_local
    rows = bands * sub_local * times * 2
    vmem = pl.BlockSpec(memory_space=pltpu.VMEM)
    anywhere = pl.BlockSpec(memory_space=pl.ANY)

    sent = pl.pallas_call(
        functools.partial(front_kernel, times, blocks, near, beams),
        out_shape=jax.ShapeDtypeStruct((peers, tall, times * beams), BF16),
        in_specs=[vmem] * 3,
        out_specs=vmem,
        scratch_shapes=[pltpu.VMEM((GX, 2 * GY // LANES, rows, LANES), F32)],
        cost_estimate=pl.CostEstimate(flops=2 * 10**9, bytes_accessed=4 * 10**6, transcendentals=0),
        name="front",
    )(voltages.reshape(rows // 2, 2, feeds), grid_feed.reshape(1, feeds), jnp.asarray(steering_table(GY)))
    own = lax.all_to_all(sent, ("far", "near", "beam"), split_axis=0, concat_axis=0, tiled=True)
    share = near // columns
    fetched = []
    for j in range(share):
        steps = [(n, x, (n + x * share + j) % near) for n in range(near) for x in range(columns)]
        pairs = [(source * columns + x, n * columns + x) for n, x, source in steps]
        fetched.append(lax.ppermute(delays, ("near", "beam"), pairs))
    lags = jnp.concatenate(fetched).astype(BF16).reshape(share, peers, sub_local, trials)
    lags = jnp.transpose(lags, (0, 3, 2, 1)).reshape(share, trials, subs)
    lags = lax.all_gather(lags, "beam").reshape(near, trials, subs)
    other = lax.ppermute(own, "dm", [(0, 1), (1, 0)])
    place = jnp.stack([lax.axis_index("dm"), lax.axis_index("near")]).astype(jnp.int32)
    local, total = pl.pallas_call(
        functools.partial(dedisperse_kernel, beams),
        out_shape=(
            jax.ShapeDtypeStruct((bands // blocks, trials, times * beams), F32),
            jax.ShapeDtypeStruct((trials, times * beams), F32),
        ),
        in_specs=[pl.BlockSpec(memory_space=pltpu.SMEM)] + [vmem] * 3,
        out_specs=(vmem, vmem),
        scratch_shapes=[
            pltpu.VMEM((2 * times * beams // LANES, peers * tall, LANES), F32),
        ],
        compiler_params=pltpu.CompilerParams(vmem_limit_bytes=24 * 2**20),
        cost_estimate=pl.CostEstimate(flops=2 * 10**9, bytes_accessed=4 * 10**6, transcendentals=0),
        name="dedisperse",
    )(place, own, other, lags)
    inner = lax.ppermute(total.astype(BF16), "far", [(k, k + 1) for k in range(0, blocks, 2)]).astype(F32)
    through = total + inner
    known = through.astype(BF16)
    before = lax.ppermute(known, "far", [(1, 3)]).astype(F32)
    handed = lax.ppermute(known, "far", [(1, 2)]).astype(F32)
    for k in range(3, blocks - 2, 2):
        before = before + lax.ppermute((before + through).astype(BF16), "far", [(k, k + 2)]).astype(F32)
    later = lax.ppermute((before + through).astype(BF16), "far", [(k, k + 1) for k in range(3, blocks - 1, 2)])
    base = inner + before + handed + later.astype(F32)
    cumulative = (local + base).astype(BF16)
    slabs = lax.all_to_all(cumulative, "near", split_axis=0, concat_axis=0, tiled=True)
    spread = pl.pallas_call(
        functools.partial(spread_kernel, beams, 1.0 / math.sqrt(FREQS)),
        out_shape=jax.ShapeDtypeStruct((trials * times * near * beams // LANES, LANES), F32),
        in_specs=[vmem],
        out_specs=vmem,
        compiler_params=pltpu.CompilerParams(vmem_limit_bytes=24 * 2**20),
        name="spread",
    )(slabs)
    spread = jnp.transpose(spread.reshape(trials, near * beams // LANES, times, LANES), (0, 2, 1, 3))
    return spread.reshape(1, trials, times, near * beams)


def solution(mesh):
    near = 4
    sizes = mesh.shape
    devices = mesh.devices.reshape(sizes["grp"], sizes["freq"] // near, near, sizes["beam"], sizes["dm"])
    split = Mesh(devices, ("grp", "far", "near", "beam", "dm"))
    freq = ("far", "near")
    in_specs = (P(None, (*freq, "beam"), ("grp", "dm"), None, None), P(), P(freq, None, "dm"))
    out_specs = P(freq, "dm", "grp", "beam")
    return jax.shard_map(search, mesh=split, in_specs=in_specs, out_specs=out_specs, check_vma=False)
```

```python
import functools
import math

import jax
import jax.numpy as jnp
import numpy as np
from jax import lax
from jax.experimental import pallas as pl
from jax.experimental.pallas import tpu as pltpu
from jax.sharding import Mesh
from jax.sharding import PartitionSpec as P


GX = 4
GY = 256
FREQS = 8192
LAGS = 5
LANES = 128
BF16 = jnp.bfloat16
F32 = jnp.float32


def steering_table(length):
    position = np.arange(length)
    angle = (position[:, None] * position[None, :] % length) * (2.0 * math.pi / length)
    cosine = np.cos(angle) / math.sqrt(length)
    sine = np.sin(angle) / math.sqrt(length)
    upper = np.concatenate([cosine, -sine], axis=1)
    lower = np.concatenate([sine, cosine], axis=1)
    return np.concatenate([upper, lower], axis=0).astype(BF16)


def iota(shape, dim):
    return lax.broadcasted_iota(jnp.int32, shape, dim)


def lane_blocks(arrays, width, shift):
    count = len(arrays)
    block = iota(arrays[0].shape, 1) // width
    result = None
    for i, array in enumerate(arrays):
        amount = (i - shift) % count * width
        moved = pltpu.roll(array, amount, 1) if amount else array
        result = moved if result is None else jnp.where(block == i, moved, result)
    return result


def front_kernel(times, blocks, near, beams, volt_ref, feed_ref, table_ref, out_ref, along_ref):
    rows, feeds = 2 * volt_ref.shape[0], volt_ref.shape[2]
    chans = rows // (2 * times)
    tall = chans // blocks
    pick = jnp.where(iota((feeds, feeds), 0) == feed_ref[...], 1.0, 0.0).astype(BF16)
    volts = volt_ref[...].reshape(rows, feeds)
    grid = jnp.dot(volts, pick, preferred_element_type=F32).astype(BF16)
    table = table_ref[pl.ds(GY, GY), :]
    halves = GY // LANES
    for gx in range(GX):
        along = jnp.dot(grid[:, gx * GY : (gx + 1) * GY], table, preferred_element_type=F32)
        for u in range(2 * halves):
            along_ref[gx, u] = along[:, u * LANES : (u + 1) * LANES]
    per_tile = LANES // beams
    group = max(tall, 16)
    for first in range(0, chans, group):
        for tile in range(GY // LANES):
            power = [[] for _ in range(GX)]
            for t in range(times):
                r0, r1 = (pl.ds((first * times + t) * 2 + p, group, stride=2 * times) for p in range(2))
                re, im = [], []
                for gx in range(GX):
                    sine, cosine = along_ref.at[gx, tile], along_ref.at[gx, halves + tile]
                    re.append((cosine[r0, :] + sine[r1, :]).astype(BF16).astype(F32))
                    im.append((cosine[r1, :] - sine[r0, :]).astype(BF16).astype(F32))
                er, ei, orr, oi = re[0] + re[2], im[0] + im[2], re[1] + re[3], im[1] + im[3]
                dr, di, ur, ui = re[0] - re[2], im[0] - im[2], re[1] - re[3], im[1] - im[3]
                formed = [(er + orr, ei + oi), (dr + ui, di - ur), (er - orr, ei - oi), (dr - ui, di + ur)]
                for bx, (fr, fi) in enumerate(formed):
                    fr, fi = 0.5 * fr, 0.5 * fi
                    power[bx].append(0.5 * (fr * fr + fi * fi))
            for bx in range(GX):
                for part in range(per_tile):
                    slab = tile * per_tile + part
                    for u in range(times // per_tile):
                        packed = lane_blocks(power[bx][u * per_tile : (u + 1) * per_tile], beams, part)
                        for row in range(0, group, tall):
                            peer = ((first + row) // tall * near + slab) * GX + bx
                            out_ref[peer, :, pl.ds(u * LANES, LANES)] = packed[row : row + tall].astype(BF16)


def dedisperse_kernel(beams, place_ref, own_ref, other_ref, lag_ref, out_ref, total_ref, level_ref):
    sources, tall, width = own_ref.shape
    bands = out_ref.shape[0]
    subs = tall // bands
    chunk = 8
    low = place_ref[0] == 0

    tiles = width // LANES

    def center(i, carry):
        mine = own_ref[pl.ds(i * chunk, chunk)].astype(F32).reshape(chunk * tall, width)
        theirs = other_ref[pl.ds(i * chunk, chunk)].astype(F32).reshape(chunk * tall, width)
        levels = []
        for half in (jnp.where(low, mine, theirs), jnp.where(low, theirs, mine)):
            levels += [half[:, u * LANES : (u + 1) * LANES] for u in range(tiles)]
        total = sum(levels[1:], levels[0])
        amount = LANES // 2
        while amount >= beams:
            total = total + pltpu.roll(total, amount, 1)
            amount //= 2
        mean = total * (0.5 * beams / width)
        r = pl.ds(pl.multiple_of(i * (chunk * tall), chunk * tall), chunk * tall)
        for u, level in enumerate(levels):
            level_ref[u, r, :] = level - mean
        return carry

    lax.fori_loop(0, sources // chunk, center, 0)
    lane = iota((out_ref.shape[1], LANES), 1)
    running = [None] * tiles
    for b in range(bands):
        rows = []
        for s in range(subs):
            r = pl.ds(b * subs + s, sources, stride=tall)
            rows.append(jnp.concatenate([level_ref[u, r, :].astype(BF16) for u in range(2 * tiles)], axis=1))
        data = jnp.concatenate(rows, axis=0)
        lags = lag_ref[lax.rem(b + bands - place_ref[1], bands)].astype(F32)
        for v in range(LAGS):
            chosen = jnp.where(lags == float(v), 1.0, 0.0).astype(BF16)
            picked = jnp.dot(chosen, data, preferred_element_type=F32)
            for u in range(tiles):
                whole, rest = divmod(v * beams + u * LANES, LANES)
                part = picked[:, whole * LANES : (whole + 1) * LANES]
                if rest:
                    after = picked[:, (whole + 1) * LANES : (whole + 2) * LANES]
                    back = LANES - rest
                    part = jnp.where(lane < back, pltpu.roll(part, back, 1), pltpu.roll(after, back, 1))
                running[u] = part if running[u] is None else running[u] + part
        for u in range(tiles):
            out_ref[b, :, pl.ds(u * LANES, LANES)] = running[u]
    for u in range(tiles):
        total_ref[:, pl.ds(u * LANES, LANES)] = running[u]


def spread_kernel(beams, scale, in_ref, out_ref):
    slabs, trials, width = in_ref.shape
    times = width // beams
    count = LANES // beams
    stride = slabs // count * times
    for tile in range(slabs // count):
        for t in range(times):
            source, shift = t * beams // LANES, t * beams % LANES // beams
            cut = pl.ds(source * LANES, LANES)
            parts = [in_ref[tile * count + i, :, cut].astype(F32) * scale for i in range(count)]
            out_ref[pl.ds(tile * times + t, trials, stride=stride), :] = lane_blocks(parts, beams, shift)


def search(voltages, grid_feed, delays):
    bands, sub_local, times = voltages.shape[:3]
    feeds = voltages.shape[4]
    blocks, near, columns = lax.axis_size("far"), lax.axis_size("near"), lax.axis_size("beam")
    peers = blocks * near * columns
    beams = feeds // columns // near
    trials = delays.shape[2]
    subs = delays.shape[1]
    tall = bands // blocks * sub_local
    rows = bands * sub_local * times * 2
    vmem = pl.BlockSpec(memory_space=pltpu.VMEM)
    anywhere = pl.BlockSpec(memory_space=pl.ANY)

    sent = pl.pallas_call(
        functools.partial(front_kernel, times, blocks, near, beams),
        out_shape=jax.ShapeDtypeStruct((peers, tall, times * beams), BF16),
        in_specs=[vmem] * 3,
        out_specs=vmem,
        scratch_shapes=[pltpu.VMEM((GX, 2 * GY // LANES, rows, LANES), F32)],
        cost_estimate=pl.CostEstimate(flops=2 * 10**9, bytes_accessed=4 * 10**6, transcendentals=0),
        name="front",
    )(voltages.reshape(rows // 2, 2, feeds), grid_feed.reshape(1, feeds), jnp.asarray(steering_table(GY)))
    own = lax.all_to_all(sent, ("far", "near", "beam"), split_axis=0, concat_axis=0, tiled=True)
    lags = delays.astype(BF16).reshape(peers, sub_local, trials)
    lags = [jnp.transpose(lags, (2, 1, 0)).reshape(trials, subs)]
    for j in range(1, near):
        lags.append(lax.ppermute(lags[0], "near", [((n + j) % near, n) for n in range(near)]))
    lags = jnp.stack(lags)
    other = lax.ppermute(own, "dm", [(0, 1), (1, 0)])
    place = jnp.stack([lax.axis_index("dm"), lax.axis_index("near")]).astype(jnp.int32)
    local, total = pl.pallas_call(
        functools.partial(dedisperse_kernel, beams),
        out_shape=(
            jax.ShapeDtypeStruct((bands // blocks, trials, times * beams), F32),
            jax.ShapeDtypeStruct((trials, times * beams), F32),
        ),
        in_specs=[pl.BlockSpec(memory_space=pltpu.SMEM)] + [vmem] * 3,
        out_specs=(vmem, vmem),
        scratch_shapes=[
            pltpu.VMEM((2 * times * beams // LANES, peers * tall, LANES), F32),
        ],
        compiler_params=pltpu.CompilerParams(vmem_limit_bytes=24 * 2**20),
        cost_estimate=pl.CostEstimate(flops=2 * 10**9, bytes_accessed=4 * 10**6, transcendentals=0),
        name="dedisperse",
    )(place, own, other, lags)
    inner = lax.ppermute(total.astype(BF16), "far", [(k, k + 1) for k in range(0, blocks, 2)]).astype(F32)
    through = total + inner
    known = through.astype(BF16)
    before = lax.ppermute(known, "far", [(1, 3)]).astype(F32)
    handed = lax.ppermute(known, "far", [(1, 2)]).astype(F32)
    for k in range(3, blocks - 2, 2):
        before = before + lax.ppermute((before + through).astype(BF16), "far", [(k, k + 2)]).astype(F32)
    later = lax.ppermute((before + through).astype(BF16), "far", [(k, k + 1) for k in range(3, blocks - 1, 2)])
    base = inner + before + handed + later.astype(F32)
    cumulative = (local + base).astype(BF16)
    slabs = lax.all_to_all(cumulative, "near", split_axis=0, concat_axis=0, tiled=True)
    spread = pl.pallas_call(
        functools.partial(spread_kernel, beams, 1.0 / math.sqrt(FREQS)),
        out_shape=jax.ShapeDtypeStruct((trials * times * near * beams // LANES, LANES), F32),
        in_specs=[vmem],
        out_specs=vmem,
        compiler_params=pltpu.CompilerParams(vmem_limit_bytes=24 * 2**20),
        name="spread",
    )(slabs)
    spread = jnp.transpose(spread.reshape(trials, near * beams // LANES, times, LANES), (0, 2, 1, 3))
    return spread.reshape(1, trials, times, near * beams)


def solution(mesh):
    near = 4
    sizes = mesh.shape
    devices = mesh.devices.reshape(sizes["grp"], sizes["freq"] // near, near, sizes["beam"], sizes["dm"])
    split = Mesh(devices, ("grp", "far", "near", "beam", "dm"))
    freq = ("far", "near")
    in_specs = (P(None, (*freq, "beam"), ("grp", "dm"), None, None), P(), P(freq, None, "dm"))
    out_specs = P(freq, "dm", "grp", "beam")
    return jax.shard_map(search, mesh=split, in_specs=in_specs, out_specs=out_specs, check_vma=False)
```
